32 devices in a mesh: tm: 8 (over y, x, core), sr: 4 (over z).
Axes of the slice: x: 2, y: 2, z: 4, core: 2. Of those that a mesh axis runs over, the one named last changes fastest.
Arguments:
- observations: bfloat16 [1024, 65536], P(None, ('sr', 'tm')), may hold values from -6 to 6
- loadings: float32 [65536, 128], P(('sr', 'tm')), may hold values from -0.0007324219 to 0.0007324219
- noise_precision: float32 [65536], P(('sr', 'tm')), may hold values from 0.5 to 4
- transition: float32 [128, 128], replicated, may hold values from -1 to 1, as said below
- filter_cov: float32 [128, 128], replicated, may hold values from -1 to 1, as said below
- smoother_gain: float32 [128, 128], replicated, may hold values from -1 to 1, as said below
- smoothed_cov: float32 [128, 128], replicated, may hold values from -1 to 1, as said below
Outputs:
- smoothed_factors: float32 [1024, 128], P('tm')
- new_loadings: float32 [65536, 128], P(('sr', 'tm'))
- new_transition: float32 [128, 128], replicated
The draws below stay inside these ranges and needn't reach their ends.
Inputs may be any that keep to these rules, and one draw needn't show every extreme that they name: `transition`: the spectral radius is below one. `filter_cov`: symmetric positive definite. `smoother_gain`: the spectral radius is below one. `smoothed_cov`: symmetric positive definite.
All inputs are finite; a program needn't handle non-finite values.
Results may differ from the reference program's by a relative error of at most 0.00175.
The reference program's roundings to bfloat16 on the way (of `scaled` and `factors_b`) count: a program that leaves them out, or rounds other values in their place, can miss the bound.
Values may be sent and summed in bfloat16 or wider, within the bound.
A program may use at most 64 MiB of HBM per device.

```python
import math
import jax
import jax.numpy as jnp
from jax import lax

SERIES = 65536
FACTORS = 128
TIME = 1024


def modal_parts(key):
    base = jax.random.fold_in(key, 4711)
    subkeys = jax.random.split(base, 10)
    normal_basis = jax.random.normal(subkeys[0], (FACTORS, FACTORS), jnp.float32)
    basis, unused = jnp.linalg.qr(normal_basis)
    slowness = jax.random.randint(subkeys[1], (FACTORS // 2,), 0, 2) > 0
    return (basis, slowness, subkeys)


def rotation_blocks(radius, angle):
    evens = jnp.arange(0, FACTORS, 2)
    cosine = radius * jnp.cos(angle)
    sine = radius * jnp.sin(angle)
    matrix = jnp.zeros((FACTORS, FACTORS), jnp.float32)
    matrix = matrix.at[evens, evens].set(cosine).at[evens, evens + 1].set(-sine)
    matrix = matrix.at[evens + 1, evens].set(sine).at[evens + 1, evens + 1].set(cosine)
    return matrix


def turning(basis, slowness, first_key, second_key, angle_key):
    half = FACTORS // 2
    slow_radius = jnp.exp(-jax.random.uniform(first_key, (half,), jnp.float32, 0.1, 0.6) / TIME)
    fast_radius = jnp.exp(-1.0 / jax.random.uniform(second_key, (half,), jnp.float32, 30.0, 50.0))
    radius = jnp.where(slowness, slow_radius, fast_radius)
    angle = jax.random.uniform(angle_key, (half,), jnp.float32, 0.3, 2.8)
    inner = rotation_blocks(radius, angle)
    return jnp.dot(jnp.dot(basis, inner, precision=lax.Precision.HIGHEST), basis.T, precision=lax.Precision.HIGHEST)


def draw_transition(key, part):
    basis, slowness, subkeys = modal_parts(key)
    return turning(basis, slowness, subkeys[2], subkeys[3], subkeys[4])


def draw_smoother_gain(key, part):
    basis, slowness, subkeys = modal_parts(key)
    return turning(basis, slowness, subkeys[5], subkeys[6], subkeys[7])


def draw_filter_cov(key, part):
    basis, slowness, subkeys = modal_parts(key)
    values = jnp.exp(jax.random.uniform(subkeys[8], (FACTORS,), jnp.float32, jnp.log(0.2), 0.0))
    return jnp.dot(basis * values[None, :], basis.T, precision=lax.Precision.HIGHEST)


def draw_smoothed_cov(key, part):
    basis, slowness, subkeys = modal_parts(key)
    values = jax.random.uniform(subkeys[9], (FACTORS,), jnp.float32, 0.3, 1.0)
    return jnp.dot(basis * values[None, :], basis.T, precision=lax.Precision.HIGHEST)


def block_levels(own_key, extent, shards, low, top_value):
    loudness = 1.0
    for axis_at, shards_of in shards:
        draws = jax.random.uniform(jax.random.fold_in(jax.random.fold_in(own_key, 6), axis_at), (shards_of,), jnp.float32, low / len(shards), top_value / len(shards))
        loudness = loudness * jnp.repeat(jnp.exp(draws), extent[axis_at] // shards_of).reshape((-1,) + (1,) * (len(extent) - 1 - axis_at))
    return loudness


def normal_values(key, dims, width, bound, cuts=(), dtype=jnp.bfloat16):
    level = block_levels(key, dims, cuts, -0.22, 0.18) if cuts else 1.0
    values = jax.random.normal(key, dims, jnp.float32) * width * level
    return jnp.minimum(jnp.maximum(values, -bound), bound).astype(dtype)


def setup_inputs(seed: int = 0) -> dict:
    splits = jax.random.split(jax.random.key(seed), 8)
    observations = normal_values(splits[0], (TIME, SERIES), 1.0, 6.0, ((1, 32),))
    loadings = normal_values(splits[1], (SERIES, FACTORS), (SERIES * TIME) ** -0.5, 0.0007324219, ((0, 32),), jnp.float32)
    noise_precision = jnp.clip(jnp.exp(math.log(4.0) - 2.0794415 * jax.random.uniform(splits[2], (SERIES,), jnp.float32) ** block_levels(splits[2], (SERIES,), ((0, 32),), -0.2, 0.2)), 0.5, 4.0)
    transition = draw_transition(jax.random.fold_in(splits[7], 71), 0)
    filter_cov = draw_filter_cov(jax.random.fold_in(splits[7], 71), 0)
    smoother_gain = draw_smoother_gain(jax.random.fold_in(splits[7], 71), 0)
    smoothed_cov = draw_smoothed_cov(jax.random.fold_in(splits[7], 71), 0)
    return dict(observations=observations, loadings=loadings, noise_precision=noise_precision, transition=transition, filter_cov=filter_cov, smoother_gain=smoother_gain, smoothed_cov=smoothed_cov)


precise = lax.Precision.HIGHEST

def dot_high(left, right):
    return jnp.dot(left.astype(jnp.float32), right.astype(jnp.float32), precision=precise, preferred_element_type=jnp.float32)

def reference(observations, loadings, noise_precision, transition, filter_cov, smoother_gain, smoothed_cov):
    scaled = (noise_precision[:, None] * loadings).astype(jnp.bfloat16)
    proj = jnp.dot(observations.astype(jnp.float32), scaled.astype(jnp.float32), preferred_element_type=jnp.float32)
    info = dot_high(loadings.T, noise_precision[:, None] * loadings)
    closed = transition - dot_high(filter_cov, dot_high(info, transition))
    inputs = dot_high(proj, filter_cov.T)

    def forward(state, drive):
        following = dot_high(closed, state) + drive
        return (following, following)
    unused, filtered = lax.scan(forward, jnp.zeros((FACTORS,), jnp.float32), inputs)
    coupled = dot_high(smoother_gain, transition)
    back = filtered - dot_high(filtered, coupled.T)
    back = back.at[TIME - 1].set(filtered[TIME - 1])

    def backward(state, drive):
        following = dot_high(smoother_gain, state) + drive
        return (following, following)
    unused, smoothed = lax.scan(backward, jnp.zeros((FACTORS,), jnp.float32), back, reverse=True)
    factors_b = smoothed.astype(jnp.bfloat16)
    cross = jnp.einsum('ts,tk->sk', observations.astype(jnp.float32), factors_b.astype(jnp.float32), preferred_element_type=jnp.float32)
    total = dot_high(smoothed.T, smoothed) + TIME * smoothed_cov
    previous = dot_high(smoothed[:-1].T, smoothed[:-1]) + (TIME - 1) * smoothed_cov
    lagged = dot_high(smoothed[1:].T, smoothed[:-1]) + (TIME - 1) * dot_high(smoothed_cov, smoother_gain.T)
    total_factor = jnp.linalg.cholesky(total)
    new_loadings = jax.scipy.linalg.cho_solve((total_factor, True), cross.T).T
    previous_factor = jnp.linalg.cholesky(previous)
    new_transition = jax.scipy.linalg.cho_solve((previous_factor, True), lagged.T).T
    return (smoothed, new_loadings, new_transition)
```

```python
import functools
import jax
import jax.numpy as jnp
from jax import lax
from jax.experimental import pallas as pl
from jax.experimental.pallas import tpu as pltpu
from jax.sharding import PartitionSpec as P

precise = lax.Precision.HIGHEST
MESH = pl.DeviceIdType.MESH
SLABS = 8
PIECES = 2
PIVOTS = 4


def dot_high(left, right):
    return jnp.dot(left, right, precision=precise, preferred_element_type=jnp.float32)


def dot_first(left, right):
    return lax.dot_general(
        left, right, (((0,), (0,)), ((), ())), precision=precise, preferred_element_type=jnp.float32
    )


def halves(value):
    high = value.astype(jnp.bfloat16)
    low = (value - high.astype(jnp.float32)).astype(jnp.bfloat16)
    return high, low


def weights(matrix):
    high, low = halves(matrix)
    side = jnp.concatenate([high, low], axis=1)
    return jnp.concatenate([side, side], axis=0)


def times(value, doubled):
    high, low = halves(value)
    width = value.shape[1]
    out = jnp.dot(
        jnp.concatenate([high, low], axis=1), doubled, preferred_element_type=jnp.float32
    )
    return out[:, :width] + out[:, width:]


def project_kernel(observations, loadings, precision, out):
    _, chips, rows, width = out.shape
    block = observations.shape[0] // (2 * chips)
    depth = loadings.shape[0]
    columns = [
        jnp.broadcast_to(precision[pl.ds(at, 1), :], (width, width)).T
        for at in range(depth // width)
    ]
    weighted = loadings[...] * jnp.concatenate(columns, axis=0)
    proj = jnp.dot(
        observations[...], weighted.astype(jnp.bfloat16), preferred_element_type=jnp.float32
    )
    left = jnp.concatenate(halves(loadings[...]), axis=1)
    right = jnp.concatenate(halves(weighted), axis=1)
    both = lax.dot_general(
        left, right, (((0,), (0,)), ((), ())), preferred_element_type=jnp.float32
    )
    both = both[:width] + both[width:]
    info = both[:, :width] + both[:, width:]
    share = width // (2 * chips)

    @pl.when(pl.program_id(0) == 0)
    def _():
        out[...] = jnp.zeros_like(out)

    for chip in range(chips):
        for core in range(2):
            at = 2 * chip + core
            out[core, chip, :block, :] += proj[at * block : (at + 1) * block]
            out[core, chip, block:, :] += info[at * share : (at + 1) * share]


def project(observations, loadings, noise_precision, blocks):
    length, series = observations.shape
    width = loadings.shape[1]
    depth = min(series, 512)
    lanes = depth // width
    shape = (2, blocks // 2, (length + width) // blocks, width)
    return pl.pallas_call(
        project_kernel,
        grid=(series // depth,),
        out_shape=jax.ShapeDtypeStruct(shape, jnp.float32),
        in_specs=[
            pl.BlockSpec((length, depth), lambda at: (0, at)),
            pl.BlockSpec((depth, width), lambda at: (at, 0)),
            pl.BlockSpec((None, lanes, width), lambda at: (at, 0, 0)),
        ],
        out_specs=pl.BlockSpec(shape, lambda at: (0, 0, 0, 0)),
        name="project",
    )(observations, loadings, noise_precision.reshape(series // depth, lanes, width))


def reduce_kernel(
    chips, planes, pieces, part, out, pair_in, mine, chip_in, plane_in,
    pair_send, pair_recv, chip_send, chip_recv, plane_send, plane_recv,
    back_send, back_recv, last_send, last_recv,
):
    tm = lax.axis_index("tm")
    sr = lax.axis_index("sr")
    core = lax.rem(tm, 2)
    chip = tm // 2
    other = 1 - core
    partner = (2 * chip + other, sr)

    def chip_at(step):
        return lax.rem(chip + step, chips)

    def plane_at(step):
        return lax.rem(sr + step, planes)

    barrier = pltpu.get_barrier_semaphore()
    pl.semaphore_signal(barrier, inc=1, device_id=partner, device_id_type=MESH)
    for step in range(1, chips):
        pl.semaphore_signal(
            barrier, inc=1, device_id=(2 * chip_at(step) + core, sr), device_id_type=MESH
        )
    for step in range(1, planes):
        pl.semaphore_signal(barrier, inc=1, device_id=(tm, plane_at(step)), device_id_type=MESH)
    pl.semaphore_wait(barrier, 1 + chips - 1 + planes - 1)

    order = list(range(1, chips)) + [0]
    pairs, across, along, back, last = {}, {}, {}, {}, {}
    for at, rows in enumerate(pieces):
        for step in order:
            target = chip_at(step)
            pairs[at, step] = pltpu.make_async_remote_copy(
                src_ref=part.at[other, target, rows],
                dst_ref=pair_in.at[step, rows],
                send_sem=pair_send.at[at, step],
                recv_sem=pair_recv.at[at, step],
                device_id=partner,
                device_id_type=MESH,
            )
            pairs[at, step].start()
    for at, rows in enumerate(pieces):
        for step in order:
            pairs[at, step].wait_recv()
            mine[step, rows] = part[core, chip_at(step), rows] + pair_in[step, rows]
            if step > 0:
                across[at, step] = pltpu.make_async_remote_copy(
                    src_ref=mine.at[step, rows],
                    dst_ref=chip_in.at[step, rows],
                    send_sem=chip_send.at[at, step],
                    recv_sem=chip_recv.at[at, step],
                    device_id=(2 * chip_at(step) + core, sr),
                    device_id_type=MESH,
                )
                across[at, step].start()
    for at, rows in enumerate(pieces):
        total = mine[0, rows]
        for step in range(1, chips):
            across[at, step].wait_recv()
            total = total + chip_in[step, rows]
        plane_in[sr, rows] = total
        for step in range(1, planes):
            along[at, step] = pltpu.make_async_remote_copy(
                src_ref=plane_in.at[sr, rows],
                dst_ref=plane_in.at[sr, rows],
                send_sem=plane_send.at[at, step],
                recv_sem=plane_recv.at[at, step],
                device_id=(tm, plane_at(step)),
                device_id_type=MESH,
            )
            along[at, step].start()

    def pass_on(at, rows, step):
        source = lax.rem(chip - step + chips, chips)
        last[at, step] = pltpu.make_async_remote_copy(
            src_ref=out.at[core, source, rows],
            dst_ref=out.at[core, source, rows],
            send_sem=last_send.at[at, step],
            recv_sem=last_recv.at[at, step],
            device_id=partner,
            device_id_type=MESH,
        )
        last[at, step].start()

    for at, rows in enumerate(pieces):
        for step in range(1, planes):
            along[at, step].wait_recv()
        whole = plane_in[0, rows]
        for plane in range(1, planes):
            whole = whole + plane_in[plane, rows]
        out[core, chip, rows] = whole
        for step in range(1, chips):
            back[at, step] = pltpu.make_async_remote_copy(
                src_ref=out.at[core, chip, rows],
                dst_ref=out.at[core, chip, rows],
                send_sem=back_send.at[at, step],
                recv_sem=back_recv.at[at, step],
                device_id=(2 * chip_at(step) + core, sr),
                device_id_type=MESH,
            )
            back[at, step].start()
        pass_on(at, rows, 0)
    for at, rows in enumerate(pieces):
        for step in range(1, chips):
            back[at, step].wait_recv()
            pass_on(at, rows, step)
    for copy in last.values():
        copy.wait_recv()
    for copies in (pairs, across, along, back, last):
        for copy in copies.values():
            copy.wait_send()


def all_sum(part, planes):
    _, chips, rows, width = part.shape
    dma = pltpu.SemaphoreType.DMA
    cuts = [rows * at // PIECES // 8 * 8 for at in range(PIECES)] + [rows]
    pieces = [slice(start, stop) for start, stop in zip(cuts, cuts[1:])]
    vmem = pl.BlockSpec(memory_space=pltpu.VMEM)
    return pl.pallas_call(
        functools.partial(reduce_kernel, chips, planes, pieces),
        out_shape=jax.ShapeDtypeStruct(part.shape, jnp.float32),
        in_specs=[vmem],
        out_specs=vmem,
        scratch_shapes=[
            pltpu.VMEM((chips, rows, width), jnp.float32),
            pltpu.VMEM((chips, rows, width), jnp.float32),
            pltpu.VMEM((chips, rows, width), jnp.float32),
            pltpu.VMEM((planes, rows, width), jnp.float32),
        ]
        + [dma((PIECES, chips))] * 4
        + [dma((PIECES, planes))] * 2
        + [dma((PIECES, chips))] * 4,
        compiler_params=pltpu.CompilerParams(collective_id=0, has_side_effects=True),
        name="all_sum",
    )(part)


def shift_rows(value, steps):
    length = value.shape[0]
    row = lax.broadcasted_iota(jnp.int32, value.shape, 0)
    moved = pltpu.roll(value, steps % length, 0)
    keep = row >= steps if steps > 0 else row < length + steps
    return jnp.where(keep, moved, 0.0)


def powers(matrix, count):
    low = [matrix]
    while len(low) < SLABS:
        low = low + [dot_high(low[-1], each) for each in low]
    high = []
    square = low[-1]
    for _ in range(count - 1):
        square = dot_high(square, square)
        high.append(square)
    return [weights(each) for each in low], [weights(low[-1])] + [weights(each) for each in high]


def scan_slabs(slabs, low, high, reverse):
    order = list(range(SLABS))[::-1] if reverse else list(range(SLABS))
    sign = -1 if reverse else 1
    part = {order[0]: slabs[order[0]]}
    for before, now in zip(order, order[1:]):
        part[now] = slabs[now] + times(part[before], low[0])
    ends = part[order[-1]]
    for level, power in enumerate(high):
        ends = ends + times(shift_rows(ends, sign * 2**level), power)
    carry = shift_rows(ends, sign)
    out = [None] * SLABS
    for place, now in enumerate(order[:-1]):
        out[now] = part[now] + times(carry, low[place])
    out[order[-1]] = ends
    return out


def inverse_two(a, b, c):
    scale = 1.0 / (a * c - b * b)
    return c * scale, -b * scale, a * scale


def inverse_four(p):
    e, f, g = inverse_two(p[0][0], p[0][1], p[1][1])
    u00 = e * p[0][2] + f * p[1][2]
    u01 = e * p[0][3] + f * p[1][3]
    u10 = f * p[0][2] + g * p[1][2]
    u11 = f * p[0][3] + g * p[1][3]
    s00 = p[2][2] - (p[0][2] * u00 + p[1][2] * u10)
    s01 = p[2][3] - (p[0][2] * u01 + p[1][2] * u11)
    s11 = p[3][3] - (p[0][3] * u01 + p[1][3] * u11)
    t00, t01, t11 = inverse_two(s00, s01, s11)
    v00 = u00 * t00 + u01 * t01
    v01 = u00 * t01 + u01 * t11
    v10 = u10 * t00 + u11 * t01
    v11 = u10 * t01 + u11 * t11
    a00 = e + (v00 * u00 + v01 * u01)
    a01 = f + (v00 * u10 + v01 * u11)
    a11 = g + (v10 * u10 + v11 * u11)
    return [
        [a00, a01, -v00, -v01],
        [a01, a11, -v10, -v11],
        [-v00, -v10, t00, t01],
        [-v01, -v11, t01, t11],
    ]


def dot_last(left, right):
    return lax.dot_general(left, right, (((1,), (1,)), ((), ())), precision=precise, preferred_element_type=jnp.float32)


def pick(value, lane, half, at):
    index = jnp.where(lane >= half, half + at, at)
    return jnp.take_along_axis(value, index, axis=1, mode="promise_in_bounds")

def sweep(packed):
    half, size = packed.shape
    lane = lax.broadcasted_iota(jnp.int32, (8, size), 1)
    inner = jnp.where(lane >= half, lane - half, lane)
    sub = lax.broadcasted_iota(jnp.int32, (8, size), 0)
    groups = half // 8
    value = [packed[8 * g : 8 * g + 8] for g in range(groups)]

    def spread(tile, at):
        return jnp.broadcast_to(tile[at : at + 1, :], (8, size))

    first = [pick(value[0], lane, half, j) for j in range(PIVOTS)]
    block = [[spread(first[max(i, j)], min(i, j)) for j in range(PIVOTS)] for i in range(PIVOTS)]
    for k in range(0, half, PIVOTS):
        group, place = divmod(k, 8)
        solved = inverse_four(block)
        order = list(range(groups))
        following = k + PIVOTS
        if following < half:
            ahead, spot = divmod(following, 8)
            order.remove(ahead)
            order.insert(0, ahead)
        columns = [None] * groups
        for g in order:
            columns[g] = [pick(value[g], lane, half, k + j) for j in range(PIVOTS)]
            if g == order[0] and following < half:
                coming = [pick(value[g], lane, half, following + j) for j in range(PIVOTS)]
        if following < half:
            cross = [[spread(columns[ahead][j], spot + i) for j in range(PIVOTS)] for i in range(PIVOTS)]
            moved = [[sum(solved[i][j] * cross[b][j] for j in range(PIVOTS)) for b in range(PIVOTS)] for i in range(PIVOTS)]
            block = [[None] * PIVOTS for _ in range(PIVOTS)]
            for a in range(PIVOTS):
                for b in range(a, PIVOTS):
                    take = sum(cross[a][i] * moved[i][b] for i in range(PIVOTS))
                    block[a][b] = block[b][a] = spread(coming[b], spot + a) - take
        here = (inner >= k) & (inner < k + PIVOTS)
        rows = []
        for i in range(PIVOTS):
            row = jnp.where(here, 0.0, spread(value[group], place + i))
            rows.append(jnp.where(inner == k + i, 1.0, row))
        fresh = [sum(solved[i][j] * rows[j] for j in range(PIVOTS)) for i in range(PIVOTS)]
        updated = [None] * groups
        for g in order:
            take = sum(columns[g][i] * fresh[i] for i in range(PIVOTS))
            updated[g] = jnp.where(here, 0.0, value[g]) - take
            if g == group:
                for i in range(PIVOTS):
                    updated[g] = jnp.where(sub == place + i, fresh[i], updated[g])
        value = updated
    return jnp.concatenate(value, axis=0)


def invert(matrices):
    size = matrices[0].shape[0]
    half = size // 2
    row_at = lax.broadcasted_iota(jnp.int32, (size, size), 0)
    lane_at = lax.broadcasted_iota(jnp.int32, (size, size), 1)
    low = lax.broadcasted_iota(jnp.int32, (half, size), 1) < half
    nothing = jnp.zeros((half, size), jnp.float32)
    diagonal = row_at == lane_at
    scales, scaled = [], []
    for m in matrices:
        only = jnp.where(diagonal, m, 0.0)
        across = lax.rsqrt(jnp.sum(only, axis=0, keepdims=True))
        down = lax.rsqrt(jnp.sum(only, axis=1, keepdims=True))
        scales.append((across, down))
        scaled.append((m * across) * down)
    one, two = scaled
    packed = sweep(jnp.where(low, one[:half], pltpu.roll(two[:half], half, 1)))
    corner = [jnp.where(low, packed, 0.0), jnp.where(low, pltpu.roll(packed, half, 1), 0.0)]
    upper, rest = [], []
    for m, each in zip(scaled, corner):
        over = jnp.where(low, 0.0, dot_high(each, m))
        over = jnp.concatenate([over, nothing], axis=0)
        upper.append(over)
        rest.append(m[half:] - dot_high(jnp.where(low, m[half:], 0.0), over))
    packed = sweep(jnp.where(low, pltpu.roll(rest[1], half, 1), rest[0]))
    final = [jnp.where(low, 0.0, packed), jnp.where(low, 0.0, pltpu.roll(packed, half, 1))]
    out = []
    for each, over, last, (across, down) in zip(corner, upper, final, scales):
        side = dot_high(over[:half], jnp.concatenate([nothing, last], axis=0))
        top = each + dot_last(side, over) - side
        bottom = last - dot_last(last, over)
        out.append((jnp.concatenate([top, bottom], axis=0) * across) * down)
    return out


def smooth_kernel(
    total_in, transition, filter_cov, gain, cov, observations, own, updated, moved,
    drive, held, arrived,
):
    length = observations.shape[0]
    panel = pltpu.make_async_copy(observations, held, arrived)
    panel.start()
    width = transition.shape[0]
    _, chips, rows, _ = total_in.shape
    block = length // (2 * chips)
    count = length // SLABS
    levels = (count - 1).bit_length()
    info = jnp.concatenate(
        [total_in[core, chip, block:, :] for chip in range(chips) for core in range(2)], axis=0
    )
    closed = transition[...] - dot_high(filter_cov[...], dot_high(info, transition[...]))
    low, high = powers(closed.T, levels)
    cov_t = weights(filter_cov[...].T)
    for chip in range(chips):
        for core in range(2):
            start = (2 * chip + core) * block
            drive[start : start + block, :] = times(total_in[core, chip, :block, :], cov_t)
    slabs = [drive[pl.ds(at, count, stride=SLABS), :] for at in range(SLABS)]
    filtered = scan_slabs(slabs, low, high, False)
    coupled = weights(dot_high(gain[...], transition[...]).T)
    last = lax.broadcasted_iota(jnp.int32, (count, width), 0) == count - 1
    back = [each - times(each, coupled) for each in filtered]
    back[-1] = jnp.where(last, filtered[-1], back[-1])
    low, high = powers(gain[...].T, levels)
    smooth = scan_slabs(back, low, high, True)
    for at in range(SLABS):
        drive[pl.ds(at, count, stride=SLABS), :] = smooth[at]
    place = pl.multiple_of(lax.axis_index("tm") * block, block)
    own[...] = drive[pl.ds(place, block), :]
    whole = drive[...]
    high, rest = halves(whole)
    factors = high.T
    time = lax.broadcasted_iota(jnp.int32, whole.shape, 0)
    kept = halves(jnp.where(time == length - 1, 0.0, whole))
    lag = halves(shift_rows(whole, 1))
    sums = jnp.dot(
        jnp.concatenate([factors, rest.T], axis=0),
        jnp.concatenate(kept + lag, axis=1),
        preferred_element_type=jnp.float32,
    )
    sums = sums[:width] + sums[width:]
    previous = sums[:, :width] + sums[:, width : 2 * width]
    lagged = sums[:, 2 * width : 3 * width] + sums[:, 3 * width :]
    final = smooth[-1][count - 8 :, :]
    final = jnp.where(lax.broadcasted_iota(jnp.int32, final.shape, 0) == 7, final, 0.0)
    total = previous + dot_first(final, final)
    total = total + length * cov[...]
    previous = previous + (length - 1) * cov[...]
    lagged = lagged + (length - 1) * dot_high(cov[...], gain[...].T)
    panel.wait()
    series = updated.shape[0]
    parts = [slice(start, min(start + 256, series)) for start in range(0, series, 256)]
    for part in parts:
        updated[part, :] = jnp.dot(
            factors, held[:, part], preferred_element_type=jnp.float32
        ).T
    total, previous = invert([total, previous])
    total = weights(total)
    for part in parts:
        updated[part, :] = times(updated[part, :], total)
    moved[...] = dot_high(lagged, previous)


def local(
    observations, loadings, noise_precision, transition, filter_cov, smoother_gain, smoothed_cov
):
    blocks = lax.axis_size("tm")
    planes = lax.axis_size("sr")
    width = transition.shape[0]
    length = observations.shape[0]
    steps_dev = length // blocks
    part = project(observations, loadings, noise_precision, blocks)
    summed = all_sum(part, planes)
    vmem = pl.BlockSpec(memory_space=pltpu.VMEM)
    series = observations.shape[1]
    return pl.pallas_call(
        smooth_kernel,
        out_shape=[
            jax.ShapeDtypeStruct((steps_dev, width), jnp.float32),
            jax.ShapeDtypeStruct((series, width), jnp.float32),
            jax.ShapeDtypeStruct((width, width), jnp.float32),
        ],
        in_specs=[vmem] * 5 + [pl.BlockSpec(memory_space=pl.ANY)],
        out_specs=[vmem] * 3,
        scratch_shapes=[
            pltpu.VMEM((length, width), jnp.float32),
            pltpu.VMEM((length, series), observations.dtype),
            pltpu.SemaphoreType.DMA,
        ],
        name="smooth",
    )(summed, transition, filter_cov, smoother_gain, smoothed_cov, observations)


def solution(mesh):
    in_specs = (P(None, ("sr", "tm")), P(("sr", "tm"), None), P(("sr", "tm")), P(), P(), P(), P())
    out_specs = (P("tm", None), P(("sr", "tm"), None), P())
    return jax.shard_map(local, mesh=mesh, in_specs=in_specs, out_specs=out_specs, check_vma=False)
```

```python
import functools
import jax
import jax.numpy as jnp
from jax import lax
from jax.experimental import pallas as pl
from jax.experimental.pallas import tpu as pltpu
from jax.sharding import PartitionSpec as P

precise = lax.Precision.HIGHEST
MESH = pl.DeviceIdType.MESH
SLABS = 8
PIVOTS = 4


def dot_high(left, right):
    return jnp.dot(left, right, precision=precise, preferred_element_type=jnp.float32)


def dot_first(left, right):
    return lax.dot_general(
        left, right, (((0,), (0,)), ((), ())), precision=precise, preferred_element_type=jnp.float32
    )


def halves(value):
    high = value.astype(jnp.bfloat16)
    low = (value - high.astype(jnp.float32)).astype(jnp.bfloat16)
    return high, low


def weights(matrix):
    high, low = halves(matrix)
    side = jnp.concatenate([high, low], axis=1)
    return jnp.concatenate([side, side], axis=0)


def times(value, doubled):
    high, low = halves(value)
    width = value.shape[1]
    out = jnp.dot(
        jnp.concatenate([high, low], axis=1), doubled, preferred_element_type=jnp.float32
    )
    return out[:, :width] + out[:, width:]


def gather_kernel(
    blocks, planes, observations, loadings, precision, out, out_info,
    panel, rows_in, part, part_info, *scratch,
):
    chips = blocks // 2
    _, _, lows, rows, width = part.shape
    highs = planes // lows
    length, series = panel.shape
    share = part_info.shape[3]
    block = length // blocks
    steps = chips * lows
    tm = lax.axis_index("tm")
    sr = lax.axis_index("sr")
    core = lax.rem(tm, 2)
    chip = tm // 2
    other = 1 - core
    low = lax.rem(sr, lows)
    high = sr // lows
    partner = (2 * chip + other, sr)
    order = list(range(lows, steps)) + list(range(lows))[::-1]

    def chip_at(step):
        return lax.rem(chip + step // lows, chips)

    def low_at(step):
        return lax.rem(low + step % lows, lows)

    def member(step):
        return (2 * chip_at(step) + core, high * lows + low_at(step))

    def level(step):
        return (tm, lax.rem(high + step, highs) * lows + low)

    loads_done, panel_done = scratch[:2]
    pieces = loads_done.shape[0]
    depth = series // pieces
    loads = []
    for at in range(pieces):
        here = slice(at * depth, (at + 1) * depth)
        loads.append(
            pltpu.make_async_copy(loadings.at[here, :], rows_in.at[here, :], loads_done.at[at])
        )
        loads[-1].start()
    tall = 2 * block
    panels = {}
    for step in list(range(1, chips)) + [0]:
        start = pl.multiple_of(lax.rem(chip + step, chips) * tall, tall)
        panels[step] = pltpu.make_async_copy(
            observations.at[pl.ds(start, tall), :],
            panel.at[pl.ds(start, tall), :],
            panel_done.at[step],
        )
        panels[step].start()

    barrier = pltpu.get_barrier_semaphore()
    pl.semaphore_signal(barrier, inc=1, device_id=partner, device_id_type=MESH)
    for step in range(1, steps):
        pl.semaphore_signal(barrier, inc=1, device_id=member(step), device_id_type=MESH)
    for step in range(1, highs):
        pl.semaphore_signal(barrier, inc=1, device_id=level(step), device_id_type=MESH)

    both = None
    weighted = []
    for at in range(pieces):
        here = slice(at * depth, (at + 1) * depth)
        columns = [
            jnp.broadcast_to(precision[pl.ds(row, 1), :], (width, width)).T
            for row in range(at * depth // width, (at + 1) * depth // width)
        ]
        loads[at].wait()
        value = rows_in[here, :]
        scaled = value * jnp.concatenate(columns, axis=0)
        pair = halves(scaled)
        weighted.append(pair[0])
        left = jnp.concatenate(halves(value), axis=1)
        right = jnp.concatenate(pair, axis=1)
        each = lax.dot_general(
            left, right, (((0,), (0,)), ((), ())), preferred_element_type=jnp.float32
        )
        both = each if both is None else both + each
    weighted = jnp.concatenate(weighted, axis=0)
    both = both[:width] + both[width:]
    info = both[:, :width] + both[:, width:]
    for place in range(2 * steps):
        now = slice(place * share, (place + 1) * share)
        part_info[place // lows % 2, place // (2 * lows), place % lows] = info[now]
    pl.semaphore_wait(barrier, 1 + steps - 1 + highs - 1)

    class Stream:
        def __init__(self, part, out, pair_in, mine, cube_in, far_in, pair, across, far, back, last):
            self.part, self.out = part, out
            self.pair_in, self.mine, self.cube_in, self.far_in = pair_in, mine, cube_in, far_in
            self.pair, self.across, self.far, self.back, self.last = pair, across, far, back, last
            self.sent = []
            self.open = {}

        def send(self, key, source, target, semaphores, at, device):
            copy = pltpu.make_async_remote_copy(
                src_ref=source, dst_ref=target,
                send_sem=semaphores.at[0, at], recv_sem=semaphores.at[1, at],
                device_id=device, device_id_type=MESH,
            )
            copy.start()
            self.open[key] = copy
            self.sent.append(copy)

        def wait(self, key):
            self.open[key].wait_recv()

        def to_pair(self, step):
            source = self.part.at[other, chip_at(step), low_at(step)]
            self.send(("pair", step), source, self.pair_in.at[step], self.pair, step, partner)

        def to_cube(self, step):
            self.wait(("pair", step))
            self.mine[step] = self.part[core, chip_at(step), low_at(step)] + self.pair_in[step]
            if step > 0:
                self.send(
                    ("across", step), self.mine.at[step], self.cube_in.at[step],
                    self.across, step, member(step),
                )

        def to_far(self):
            total = self.mine[0]
            for step in order[:-1]:
                self.wait(("across", step))
                total = total + self.cube_in[step]
            self.far_in[high] = total
            for step in range(1, highs):
                self.send(
                    ("far", step), self.far_in.at[high], self.far_in.at[high],
                    self.far, step, level(step),
                )

        def to_back(self):
            for step in range(1, highs):
                self.wait(("far", step))
            total = self.far_in[0]
            for step in range(1, highs):
                total = total + self.far_in[step]
            here = self.out.at[core, chip, low]
            here[...] = total
            for step in order[:-1]:
                self.send(("back", step), here, here, self.back, step, member(step))
            self.send(("last", 0), here, here, self.last, 0, partner)

        def to_last(self, step):
            self.wait(("back", step))
            source = lax.rem(chip + chips - step // lows, chips)
            here = self.out.at[core, source, lax.rem(low + lows - step % lows, lows)]
            self.send(("last", step), here, here, self.last, step, partner)

    small = Stream(part_info, out_info, *scratch[2:11])
    large = Stream(part, out, *scratch[11:20])
    for step in order:
        small.to_pair(step)
    waiting = []
    for turn in list(range(1, chips)) + [0]:
        panels[turn].wait()
        source = lax.rem(chip + turn, chips)
        start = pl.multiple_of(source * tall, tall)
        proj = jnp.dot(
            panel[pl.ds(start, tall), :], weighted, preferred_element_type=jnp.float32
        )
        for at in range(2):
            for half in range(lows):
                now = slice(at * block + half * rows, at * block + (half + 1) * rows)
                part[at, source, half] = proj[now]
        fresh = [step for step in order if step // lows == turn]
        for step in fresh:
            large.to_pair(step)
        if turn == 1 % chips:
            for step in order:
                small.to_cube(step)
        for step in waiting:
            large.to_cube(step)
        waiting = fresh
    for step in waiting:
        large.to_cube(step)
    small.to_far()
    large.to_far()
    small.to_back()
    large.to_back()
    for stream in (small, large):
        for step in order[:-1]:
            stream.to_last(step)
    for stream in (small, large):
        for step in order:
            stream.wait(("last", step))
    for stream in (small, large):
        for copy in stream.sent:
            copy.wait_send()


def gather(observations, loadings, noise_precision, blocks, planes):
    length, series = observations.shape
    width = loadings.shape[1]
    chips = blocks // 2
    lows = 2 if planes % 2 == 0 else 1
    highs = planes // lows
    rows = length // (blocks * lows)
    share = width // (blocks * lows)
    pieces = min(4, series // width)
    dma = pltpu.SemaphoreType.DMA
    vmem = pl.BlockSpec(memory_space=pltpu.VMEM)
    hbm = pl.BlockSpec(memory_space=pl.ANY)
    steps = chips * lows

    def memory(*shape):
        return pltpu.VMEM(shape, jnp.float32)

    def stream(tall):
        return [memory(steps, tall, width)] * 3 + [memory(highs, tall, width)] + (
            [dma((2, steps))] * 2 + [dma((2, highs))] + [dma((2, steps))] * 2
        )

    shapes = [(2, chips, lows, tall, width) for tall in (rows, share)]
    return pl.pallas_call(
        functools.partial(gather_kernel, blocks, planes),
        out_shape=[jax.ShapeDtypeStruct(shape, jnp.float32) for shape in shapes],
        in_specs=[hbm, hbm, vmem],
        out_specs=[vmem, vmem],
        scratch_shapes=[
            pltpu.VMEM((length, series), observations.dtype),
            memory(series, width),
            memory(*shapes[0]),
            memory(*shapes[1]),
            dma((pieces,)),
            dma((chips,)),
        ]
        + stream(share)
        + stream(rows),
        compiler_params=pltpu.CompilerParams(collective_id=0, has_side_effects=True),
        name="gather",
    )(observations, loadings, noise_precision.reshape(series // width, width))


def shift_rows(value, steps):
    length = value.shape[0]
    row = lax.broadcasted_iota(jnp.int32, value.shape, 0)
    moved = pltpu.roll(value, steps % length, 0)
    keep = row >= steps if steps > 0 else row < length + steps
    return jnp.where(keep, moved, 0.0)


def powers(matrix, count):
    low = [matrix]
    while len(low) < SLABS:
        low = low + [dot_high(low[-1], each) for each in low]
    high = []
    square = low[-1]
    for _ in range(count - 1):
        square = dot_high(square, square)
        high.append(square)
    return [weights(each) for each in low], [weights(low[-1])] + [weights(each) for each in high]


def scan_slabs(slabs, low, high, reverse):
    order = list(range(SLABS))[::-1] if reverse else list(range(SLABS))
    sign = -1 if reverse else 1
    part = {order[0]: slabs[order[0]]}
    for before, now in zip(order, order[1:]):
        part[now] = slabs[now] + times(part[before], low[0])
    ends = part[order[-1]]
    for level, power in enumerate(high):
        ends = ends + times(shift_rows(ends, sign * 2**level), power)
    carry = shift_rows(ends, sign)
    out = [None] * SLABS
    for place, now in enumerate(order[:-1]):
        out[now] = part[now] + times(carry, low[place])
    out[order[-1]] = ends
    return out


def inverse_two(a, b, c):
    scale = 1.0 / (a * c - b * b)
    return c * scale, -b * scale, a * scale


def inverse_four(p):
    e, f, g = inverse_two(p[0][0], p[0][1], p[1][1])
    u00 = e * p[0][2] + f * p[1][2]
    u01 = e * p[0][3] + f * p[1][3]
    u10 = f * p[0][2] + g * p[1][2]
    u11 = f * p[0][3] + g * p[1][3]
    s00 = p[2][2] - (p[0][2] * u00 + p[1][2] * u10)
    s01 = p[2][3] - (p[0][2] * u01 + p[1][2] * u11)
    s11 = p[3][3] - (p[0][3] * u01 + p[1][3] * u11)
    t00, t01, t11 = inverse_two(s00, s01, s11)
    v00 = u00 * t00 + u01 * t01
    v01 = u00 * t01 + u01 * t11
    v10 = u10 * t00 + u11 * t01
    v11 = u10 * t01 + u11 * t11
    a00 = e + (v00 * u00 + v01 * u01)
    a01 = f + (v00 * u10 + v01 * u11)
    a11 = g + (v10 * u10 + v11 * u11)
    return [
        [a00, a01, -v00, -v01],
        [a01, a11, -v10, -v11],
        [-v00, -v10, t00, t01],
        [-v01, -v11, t01, t11],
    ]


def dot_last(left, right):
    return lax.dot_general(left, right, (((1,), (1,)), ((), ())), precision=precise, preferred_element_type=jnp.float32)


def pick(value, lane, half, at):
    index = jnp.where(lane >= half, half + at, at)
    return jnp.take_along_axis(value, index, axis=1, mode="promise_in_bounds")

def sweep(packed):
    half, size = packed.shape
    lane = lax.broadcasted_iota(jnp.int32, (8, size), 1)
    inner = jnp.where(lane >= half, lane - half, lane)
    sub = lax.broadcasted_iota(jnp.int32, (8, size), 0)
    groups = half // 8
    value = [packed[8 * g : 8 * g + 8] for g in range(groups)]

    def spread(tile, at):
        return jnp.broadcast_to(tile[at : at + 1, :], (8, size))

    first = [pick(value[0], lane, half, j) for j in range(PIVOTS)]
    block = [[spread(first[max(i, j)], min(i, j)) for j in range(PIVOTS)] for i in range(PIVOTS)]
    for k in range(0, half, PIVOTS):
        group, place = divmod(k, 8)
        solved = inverse_four(block)
        order = list(range(groups))
        following = k + PIVOTS
        if following < half:
            ahead, spot = divmod(following, 8)
            order.remove(ahead)
            order.insert(0, ahead)
        columns = [None] * groups
        for g in order:
            columns[g] = [pick(value[g], lane, half, k + j) for j in range(PIVOTS)]
            if g == order[0] and following < half:
                coming = [pick(value[g], lane, half, following + j) for j in range(PIVOTS)]
        if following < half:
            cross = [[spread(columns[ahead][j], spot + i) for j in range(PIVOTS)] for i in range(PIVOTS)]
            moved = [[sum(solved[i][j] * cross[b][j] for j in range(PIVOTS)) for b in range(PIVOTS)] for i in range(PIVOTS)]
            block = [[None] * PIVOTS for _ in range(PIVOTS)]
            for a in range(PIVOTS):
                for b in range(a, PIVOTS):
                    take = sum(cross[a][i] * moved[i][b] for i in range(PIVOTS))
                    block[a][b] = block[b][a] = spread(coming[b], spot + a) - take
        here = (inner >= k) & (inner < k + PIVOTS)
        rows = []
        for i in range(PIVOTS):
            row = jnp.where(here, 0.0, spread(value[group], place + i))
            rows.append(jnp.where(inner == k + i, 1.0, row))
        fresh = [sum(solved[i][j] * rows[j] for j in range(PIVOTS)) for i in range(PIVOTS)]
        updated = [None] * groups
        for g in order:
            take = sum(columns[g][i] * fresh[i] for i in range(PIVOTS))
            updated[g] = jnp.where(here, 0.0, value[g]) - take
            if g == group:
                for i in range(PIVOTS):
                    updated[g] = jnp.where(sub == place + i, fresh[i], updated[g])
        value = updated
    return jnp.concatenate(value, axis=0)


def invert(matrices):
    size = matrices[0].shape[0]
    half = size // 2
    row_at = lax.broadcasted_iota(jnp.int32, (size, size), 0)
    lane_at = lax.broadcasted_iota(jnp.int32, (size, size), 1)
    low = lax.broadcasted_iota(jnp.int32, (half, size), 1) < half
    nothing = jnp.zeros((half, size), jnp.float32)
    diagonal = row_at == lane_at
    scales, scaled = [], []
    for m in matrices:
        only = jnp.where(diagonal, m, 0.0)
        across = lax.rsqrt(jnp.sum(only, axis=0, keepdims=True))
        down = lax.rsqrt(jnp.sum(only, axis=1, keepdims=True))
        scales.append((across, down))
        scaled.append((m * across) * down)
    one, two = scaled
    packed = sweep(jnp.where(low, one[:half], pltpu.roll(two[:half], half, 1)))
    corner = [jnp.where(low, packed, 0.0), jnp.where(low, pltpu.roll(packed, half, 1), 0.0)]
    upper, rest = [], []
    for m, each in zip(scaled, corner):
        over = jnp.where(low, 0.0, dot_high(each, m))
        over = jnp.concatenate([over, nothing], axis=0)
        upper.append(over)
        rest.append(m[half:] - dot_high(jnp.where(low, m[half:], 0.0), over))
    packed = sweep(jnp.where(low, pltpu.roll(rest[1], half, 1), rest[0]))
    final = [jnp.where(low, 0.0, packed), jnp.where(low, 0.0, pltpu.roll(packed, half, 1))]
    out = []
    for each, over, last, (across, down) in zip(corner, upper, final, scales):
        side = dot_high(over[:half], jnp.concatenate([nothing, last], axis=0))
        top = each + dot_last(side, over) - side
        bottom = last - dot_last(last, over)
        out.append((jnp.concatenate([top, bottom], axis=0) * across) * down)
    return out


def smooth_kernel(
    total_in, info_in, transition, filter_cov, gain, cov, observations, own, updated, moved,
    drive, held, arrived,
):
    length = observations.shape[0]
    panel = pltpu.make_async_copy(observations, held, arrived)
    panel.start()
    width = transition.shape[0]
    _, chips, lows, rows, _ = total_in.shape
    count = length // SLABS
    levels = (count - 1).bit_length()
    places = [
        (core, chip, low) for chip in range(chips) for core in range(2) for low in range(lows)
    ]
    info = jnp.concatenate([info_in[place] for place in places], axis=0)
    closed = transition[...] - dot_high(filter_cov[...], dot_high(info, transition[...]))
    low, high = powers(closed.T, levels)
    cov_t = weights(filter_cov[...].T)
    for at, place in enumerate(places):
        drive[at * rows : (at + 1) * rows, :] = times(total_in[place], cov_t)
    slabs = [drive[pl.ds(at, count, stride=SLABS), :] for at in range(SLABS)]
    filtered = scan_slabs(slabs, low, high, False)
    coupled = weights(dot_high(gain[...], transition[...]).T)
    last = lax.broadcasted_iota(jnp.int32, (count, width), 0) == count - 1
    back = [each - times(each, coupled) for each in filtered]
    back[-1] = jnp.where(last, filtered[-1], back[-1])
    low, high = powers(gain[...].T, levels)
    smooth = scan_slabs(back, low, high, True)
    for at in range(SLABS):
        drive[pl.ds(at, count, stride=SLABS), :] = smooth[at]
    block = own.shape[0]
    place = pl.multiple_of(lax.axis_index("tm") * block, block)
    own[...] = drive[pl.ds(place, block), :]
    whole = drive[...]
    high, rest = halves(whole)
    factors = high.T
    time = lax.broadcasted_iota(jnp.int32, whole.shape, 0)
    kept = halves(jnp.where(time == length - 1, 0.0, whole))
    lag = halves(shift_rows(whole, 1))
    sums = jnp.dot(
        jnp.concatenate([factors, rest.T], axis=0),
        jnp.concatenate(kept + lag, axis=1),
        preferred_element_type=jnp.float32,
    )
    sums = sums[:width] + sums[width:]
    previous = sums[:, :width] + sums[:, width : 2 * width]
    lagged = sums[:, 2 * width : 3 * width] + sums[:, 3 * width :]
    final = smooth[-1][count - 8 :, :]
    final = jnp.where(lax.broadcasted_iota(jnp.int32, final.shape, 0) == 7, final, 0.0)
    total = previous + dot_first(final, final)
    total = total + length * cov[...]
    previous = previous + (length - 1) * cov[...]
    lagged = lagged + (length - 1) * dot_high(cov[...], gain[...].T)
    panel.wait()
    series = updated.shape[0]
    parts = [slice(start, min(start + 256, series)) for start in range(0, series, 256)]
    for part in parts:
        updated[part, :] = jnp.dot(
            factors, held[:, part], preferred_element_type=jnp.float32
        ).T
    total, previous = invert([total, previous])
    total = weights(total)
    for part in parts:
        updated[part, :] = times(updated[part, :], total)
    moved[...] = dot_high(lagged, previous)


def local(
    observations, loadings, noise_precision, transition, filter_cov, smoother_gain, smoothed_cov
):
    blocks = lax.axis_size("tm")
    planes = lax.axis_size("sr")
    width = transition.shape[0]
    length = observations.shape[0]
    steps_dev = length // blocks
    summed = gather(observations, loadings, noise_precision, blocks, planes)
    vmem = pl.BlockSpec(memory_space=pltpu.VMEM)
    series = observations.shape[1]
    return pl.pallas_call(
        smooth_kernel,
        out_shape=[
            jax.ShapeDtypeStruct((steps_dev, width), jnp.float32),
            jax.ShapeDtypeStruct((series, width), jnp.float32),
            jax.ShapeDtypeStruct((width, width), jnp.float32),
        ],
        in_specs=[vmem] * 6 + [pl.BlockSpec(memory_space=pl.ANY)],
        out_specs=[vmem] * 3,
        scratch_shapes=[
            pltpu.VMEM((length, width), jnp.float32),
            pltpu.VMEM((length, series), observations.dtype),
            pltpu.SemaphoreType.DMA,
        ],
        name="smooth",
    )(*summed, transition, filter_cov, smoother_gain, smoothed_cov, observations)


def solution(mesh):
    in_specs = (P(None, ("sr", "tm")), P(("sr", "tm"), None), P(("sr", "tm")), P(), P(), P(), P())
    out_specs = (P("tm", None), P(("sr", "tm"), None), P())
    return jax.shard_map(local, mesh=mesh, in_specs=in_specs, out_specs=out_specs, check_vma=False)
```

```python
import functools
import jax
import jax.numpy as jnp
from jax import lax
from jax.experimental import pallas as pl
from jax.experimental.pallas import tpu as pltpu
from jax.sharding import PartitionSpec as P

precise = lax.Precision.HIGHEST
MESH = pl.DeviceIdType.MESH
SLABS = 8
PIVOTS = 4


def dot_high(left, right):
    return jnp.dot(left, right, precision=precise, preferred_element_type=jnp.float32)


def dot_first(left, right):
    return lax.dot_general(
        left, right, (((0,), (0,)), ((), ())), precision=precise, preferred_element_type=jnp.float32
    )


def halves(value):
    high = value.astype(jnp.bfloat16)
    low = (value - high.astype(jnp.float32)).astype(jnp.bfloat16)
    return high, low


def weights(matrix):
    high, low = halves(matrix)
    side = jnp.concatenate([high, low], axis=1)
    return jnp.concatenate([side, side], axis=0)


def times(value, doubled):
    high, low = halves(value)
    width = value.shape[1]
    out = jnp.dot(
        jnp.concatenate([high, low], axis=1), doubled, preferred_element_type=jnp.float32
    )
    return out[:, :width] + out[:, width:]


def gather_kernel(
    blocks, planes, observations, loadings, precision, transition, filter_cov, gain, drive,
    near, far, out, out_info, panel, rows_in, part, part_info, *scratch,
):
    chips = blocks // 2
    _, _, lows, rows, width = part.shape
    highs = planes // lows
    length, series = panel.shape
    share = part_info.shape[3]
    block = length // blocks
    steps = chips * lows
    tm = lax.axis_index("tm")
    sr = lax.axis_index("sr")
    core = lax.rem(tm, 2)
    chip = tm // 2
    other = 1 - core
    low = lax.rem(sr, lows)
    high = sr // lows
    partner = (2 * chip + other, sr)
    order = list(range(lows, steps)) + list(range(lows))[::-1]

    def chip_at(step):
        return lax.rem(chip + step // lows, chips)

    def low_at(step):
        return lax.rem(low + step % lows, lows)

    def member(step):
        return (2 * chip_at(step) + core, high * lows + low_at(step))

    def level(step):
        return (tm, lax.rem(high + step, highs) * lows + low)

    loads_done, panel_done = scratch[:2]
    pieces = loads_done.shape[0]
    depth = series // pieces
    loads = []
    for at in range(pieces):
        here = slice(at * depth, (at + 1) * depth)
        loads.append(
            pltpu.make_async_copy(loadings.at[here, :], rows_in.at[here, :], loads_done.at[at])
        )
        loads[-1].start()
    tall = 2 * block
    panels = {}
    for step in list(range(1, chips)) + [0]:
        start = pl.multiple_of(lax.rem(chip + step, chips) * tall, tall)
        panels[step] = pltpu.make_async_copy(
            observations.at[pl.ds(start, tall), :],
            panel.at[pl.ds(start, tall), :],
            panel_done.at[step],
        )
        panels[step].start()

    barrier = pltpu.get_barrier_semaphore()
    pl.semaphore_signal(barrier, inc=1, device_id=partner, device_id_type=MESH)
    for step in range(1, steps):
        pl.semaphore_signal(barrier, inc=1, device_id=member(step), device_id_type=MESH)
    for step in range(1, highs):
        pl.semaphore_signal(barrier, inc=1, device_id=level(step), device_id_type=MESH)

    both = None
    weighted = []
    for at in range(pieces):
        here = slice(at * depth, (at + 1) * depth)
        columns = [
            jnp.broadcast_to(precision[pl.ds(row, 1), :], (width, width)).T
            for row in range(at * depth // width, (at + 1) * depth // width)
        ]
        loads[at].wait()
        value = rows_in[here, :]
        scaled = value * jnp.concatenate(columns, axis=0)
        pair = halves(scaled)
        weighted.append(pair[0])
        left = jnp.concatenate(halves(value), axis=1)
        right = jnp.concatenate(pair, axis=1)
        each = lax.dot_general(
            left, right, (((0,), (0,)), ((), ())), preferred_element_type=jnp.float32
        )
        both = each if both is None else both + each
    weighted = jnp.concatenate(weighted, axis=0)
    both = both[:width] + both[width:]
    info = both[:, :width] + both[:, width:]
    for place in range(2 * steps):
        now = slice(place * share, (place + 1) * share)
        part_info[place // lows % 2, place // (2 * lows), place % lows] = info[now]
    pl.semaphore_wait(barrier, 1 + steps - 1 + highs - 1)

    class Stream:
        def __init__(self, part, out, pair_in, mine, cube_in, far_in, pair, across, far, back, last):
            self.part, self.out = part, out
            self.pair_in, self.mine, self.cube_in, self.far_in = pair_in, mine, cube_in, far_in
            self.pair, self.across, self.far, self.back, self.last = pair, across, far, back, last
            self.sent = []
            self.open = {}

        def send(self, key, source, target, semaphores, at, device):
            copy = pltpu.make_async_remote_copy(
                src_ref=source, dst_ref=target,
                send_sem=semaphores.at[0, at], recv_sem=semaphores.at[1, at],
                device_id=device, device_id_type=MESH,
            )
            copy.start()
            self.open[key] = copy
            self.sent.append(copy)

        def wait(self, key):
            self.open[key].wait_recv()

        def to_pair(self, step):
            source = self.part.at[other, chip_at(step), low_at(step)]
            self.send(("pair", step), source, self.pair_in.at[step], self.pair, step, partner)

        def to_cube(self, step):
            self.wait(("pair", step))
            self.mine[step] = self.part[core, chip_at(step), low_at(step)] + self.pair_in[step]
            if step > 0:
                self.send(
                    ("across", step), self.mine.at[step], self.cube_in.at[step],
                    self.across, step, member(step),
                )

        def to_far(self):
            total = self.mine[0]
            for step in order[:-1]:
                self.wait(("across", step))
                total = total + self.cube_in[step]
            self.far_in[high] = total
            for step in range(1, highs):
                self.send(
                    ("far", step), self.far_in.at[high], self.far_in.at[high],
                    self.far, step, level(step),
                )

        def to_back(self):
            for step in range(1, highs):
                self.wait(("far", step))
            total = self.far_in[0]
            for step in range(1, highs):
                total = total + self.far_in[step]
            here = self.out.at[core, chip, low]
            here[...] = total
            for step in order[:-1]:
                self.send(("back", step), here, here, self.back, step, member(step))
            self.send(("last", 0), here, here, self.last, 0, partner)

        def to_last(self, step):
            self.wait(("back", step))
            source = lax.rem(chip + chips - step // lows, chips)
            here = self.out.at[core, source, lax.rem(low + lows - step % lows, lows)]
            self.send(("last", step), here, here, self.last, step, partner)

    small = Stream(part_info, out_info, *scratch[2:11])
    large = Stream(part, out, *scratch[11:20])
    for step in order:
        small.to_pair(step)
    waiting = []
    for turn in list(range(1, chips)) + [0]:
        panels[turn].wait()
        source = lax.rem(chip + turn, chips)
        start = pl.multiple_of(source * tall, tall)
        proj = jnp.dot(
            panel[pl.ds(start, tall), :], weighted, preferred_element_type=jnp.float32
        )
        for at in range(2):
            for half in range(lows):
                now = slice(at * block + half * rows, at * block + (half + 1) * rows)
                part[at, source, half] = proj[now]
        fresh = [step for step in order if step // lows == turn]
        for step in fresh:
            large.to_pair(step)
        if turn == 1 % chips:
            for step in order:
                small.to_cube(step)
        for step in waiting:
            large.to_cube(step)
        waiting = fresh
    for step in waiting:
        large.to_cube(step)
    small.to_far()
    for _ in powers(gain[...].T, near.at[1], far.at[1]):
        pass
    cov_t = weights(filter_cov[...].T)
    coupled = weights(dot_high(gain[...], transition[...]).T)
    large.to_far()
    small.to_back()
    large.to_back()
    for step in order[:-1]:
        small.to_last(step)
    for step in order:
        small.wait(("last", step))
    places = [
        (at, turn, half) for turn in range(chips) for at in range(2) for half in range(lows)
    ]
    info = jnp.concatenate([out_info[place] for place in places], axis=0)
    closed = transition[...] - dot_high(filter_cov[...], dot_high(info, transition[...]))
    for _ in powers(closed.T, near.at[0], far.at[0]):
        pass

    def enter(at, step):
        source = lax.rem(chip + chips - step // lows, chips)
        half = lax.rem(low + lows - step % lows, lows)
        start = pl.multiple_of((2 * source + at) * block + half * rows, rows)
        drive[pl.ds(start, rows), :] = times(out[at, source, half], cov_t)

    enter(core, 0)
    for step in order[:-1]:
        large.to_last(step)
        enter(core, step)
    for step in [0] + order[:-1]:
        large.wait(("last", step))
        enter(other, step)
    count = length // SLABS
    slabs = [drive[pl.ds(at, count, stride=SLABS), :] for at in range(SLABS)]
    filtered = scan_slabs(slabs, near.at[0], far.at[0], False)
    final = lax.broadcasted_iota(jnp.int32, (count, width), 0) == count - 1
    back = [each - times(each, coupled) for each in filtered]
    back[-1] = jnp.where(final, filtered[-1], back[-1])
    smooth = scan_slabs(back, near.at[1], far.at[1], True)
    for at in range(SLABS):
        drive[pl.ds(at, count, stride=SLABS), :] = smooth[at]
    for stream in (small, large):
        for copy in stream.sent:
            copy.wait_send()


def gather(observations, loadings, noise_precision, transition, filter_cov, gain, blocks, planes):
    length, series = observations.shape
    width = loadings.shape[1]
    chips = blocks // 2
    lows = 2 if planes % 2 == 0 else 1
    highs = planes // lows
    rows = length // (blocks * lows)
    share = width // (blocks * lows)
    pieces = min(4, series // width)
    dma = pltpu.SemaphoreType.DMA
    vmem = pl.BlockSpec(memory_space=pltpu.VMEM)
    hbm = pl.BlockSpec(memory_space=pl.ANY)
    steps = chips * lows
    levels = (length // SLABS - 1).bit_length()

    def memory(*shape):
        return pltpu.VMEM(shape, jnp.float32)

    def stream(tall):
        return [memory(steps, tall, width)] * 3 + [memory(highs, tall, width)] + (
            [dma((2, steps))] * 2 + [dma((2, highs))] + [dma((2, steps))] * 2
        )

    shapes = [(2, chips, lows, tall, width) for tall in (rows, share)]
    return pl.pallas_call(
        functools.partial(gather_kernel, blocks, planes),
        out_shape=jax.ShapeDtypeStruct((length, width), jnp.float32),
        in_specs=[hbm, hbm] + [vmem] * 4,
        out_specs=vmem,
        scratch_shapes=[
            pltpu.VMEM((2, SLABS - 1, 2 * width, 2 * width), jnp.bfloat16),
            pltpu.VMEM((2, levels, 2 * width, 2 * width), jnp.bfloat16),
            memory(*shapes[0]),
            memory(*shapes[1]),
            pltpu.VMEM((length, series), observations.dtype),
            memory(series, width),
            memory(*shapes[0]),
            memory(*shapes[1]),
            dma((pieces,)),
            dma((chips,)),
        ]
        + stream(share)
        + stream(rows),
        compiler_params=pltpu.CompilerParams(collective_id=0, has_side_effects=True),
        name="gather",
    )(
        observations, loadings, noise_precision.reshape(series // width, width),
        transition, filter_cov, gain,
    )


def shift_rows(value, steps):
    length = value.shape[0]
    row = lax.broadcasted_iota(jnp.int32, value.shape, 0)
    moved = pltpu.roll(value, steps % length, 0)
    keep = row >= steps if steps > 0 else row < length + steps
    return jnp.where(keep, moved, 0.0)


def powers(matrix, low, high):
    made = [matrix]
    low[0] = weights(matrix)
    while len(made) < SLABS:
        fresh = [dot_high(made[-1], each) for each in made]
        for each in fresh:
            if len(made) < SLABS - 1:
                low[len(made)] = weights(each)
            made.append(each)
        yield
    square = made[-1]
    high[0] = weights(square)
    for level in range(1, high.shape[0]):
        square = dot_high(square, square)
        high[level] = weights(square)
        yield


def scan_slabs(slabs, low, high, reverse):
    order = list(range(SLABS))[::-1] if reverse else list(range(SLABS))
    sign = -1 if reverse else 1
    part = {order[0]: slabs[order[0]]}
    for before, now in zip(order, order[1:]):
        part[now] = slabs[now] + times(part[before], low[0])
    ends = part[order[-1]]
    for level in range(high.shape[0]):
        ends = ends + times(shift_rows(ends, sign * 2**level), high[level])
    carry = shift_rows(ends, sign)
    out = [None] * SLABS
    for place, now in enumerate(order[:-1]):
        out[now] = part[now] + times(carry, low[place])
    out[order[-1]] = ends
    return out


def inverse_two(a, b, c):
    scale = 1.0 / (a * c - b * b)
    return c * scale, -b * scale, a * scale


def inverse_four(p):
    e, f, g = inverse_two(p[0][0], p[0][1], p[1][1])
    u00 = e * p[0][2] + f * p[1][2]
    u01 = e * p[0][3] + f * p[1][3]
    u10 = f * p[0][2] + g * p[1][2]
    u11 = f * p[0][3] + g * p[1][3]
    s00 = p[2][2] - (p[0][2] * u00 + p[1][2] * u10)
    s01 = p[2][3] - (p[0][2] * u01 + p[1][2] * u11)
    s11 = p[3][3] - (p[0][3] * u01 + p[1][3] * u11)
    t00, t01, t11 = inverse_two(s00, s01, s11)
    v00 = u00 * t00 + u01 * t01
    v01 = u00 * t01 + u01 * t11
    v10 = u10 * t00 + u11 * t01
    v11 = u10 * t01 + u11 * t11
    a00 = e + (v00 * u00 + v01 * u01)
    a01 = f + (v00 * u10 + v01 * u11)
    a11 = g + (v10 * u10 + v11 * u11)
    return [
        [a00, a01, -v00, -v01],
        [a01, a11, -v10, -v11],
        [-v00, -v10, t00, t01],
        [-v01, -v11, t01, t11],
    ]


def dot_last(left, right):
    return lax.dot_general(left, right, (((1,), (1,)), ((), ())), precision=precise, preferred_element_type=jnp.float32)


def pick(value, lane, half, at):
    index = jnp.where(lane >= half, half + at, at)
    return jnp.take_along_axis(value, index, axis=1, mode="promise_in_bounds")

def sweep(packed):
    half, size = packed.shape
    lane = lax.broadcasted_iota(jnp.int32, (8, size), 1)
    inner = jnp.where(lane >= half, lane - half, lane)
    sub = lax.broadcasted_iota(jnp.int32, (8, size), 0)
    groups = half // 8
    value = [packed[8 * g : 8 * g + 8] for g in range(groups)]

    def spread(tile, at):
        return jnp.broadcast_to(tile[at : at + 1, :], (8, size))

    first = [pick(value[0], lane, half, j) for j in range(PIVOTS)]
    block = [[spread(first[max(i, j)], min(i, j)) for j in range(PIVOTS)] for i in range(PIVOTS)]
    for k in range(0, half, PIVOTS):
        group, place = divmod(k, 8)
        solved = inverse_four(block)
        order = list(range(groups))
        following = k + PIVOTS
        if following < half:
            ahead, spot = divmod(following, 8)
            order.remove(ahead)
            order.insert(0, ahead)
        columns = [None] * groups
        for g in order:
            columns[g] = [pick(value[g], lane, half, k + j) for j in range(PIVOTS)]
            if g == order[0] and following < half:
                coming = [pick(value[g], lane, half, following + j) for j in range(PIVOTS)]
        if following < half:
            cross = [[spread(columns[ahead][j], spot + i) for j in range(PIVOTS)] for i in range(PIVOTS)]
            moved = [[sum(solved[i][j] * cross[b][j] for j in range(PIVOTS)) for b in range(PIVOTS)] for i in range(PIVOTS)]
            block = [[None] * PIVOTS for _ in range(PIVOTS)]
            for a in range(PIVOTS):
                for b in range(a, PIVOTS):
                    take = sum(cross[a][i] * moved[i][b] for i in range(PIVOTS))
                    block[a][b] = block[b][a] = spread(coming[b], spot + a) - take
        here = (inner >= k) & (inner < k + PIVOTS)
        rows = []
        for i in range(PIVOTS):
            row = jnp.where(here, 0.0, spread(value[group], place + i))
            rows.append(jnp.where(inner == k + i, 1.0, row))
        fresh = [sum(solved[i][j] * rows[j] for j in range(PIVOTS)) for i in range(PIVOTS)]
        updated = [None] * groups
        for g in order:
            take = sum(columns[g][i] * fresh[i] for i in range(PIVOTS))
            updated[g] = jnp.where(here, 0.0, value[g]) - take
            if g == group:
                for i in range(PIVOTS):
                    updated[g] = jnp.where(sub == place + i, fresh[i], updated[g])
        value = updated
    return jnp.concatenate(value, axis=0)


def invert(matrices):
    size = matrices[0].shape[0]
    half = size // 2
    row_at = lax.broadcasted_iota(jnp.int32, (size, size), 0)
    lane_at = lax.broadcasted_iota(jnp.int32, (size, size), 1)
    low = lax.broadcasted_iota(jnp.int32, (half, size), 1) < half
    nothing = jnp.zeros((half, size), jnp.float32)
    diagonal = row_at == lane_at
    scales, scaled = [], []
    for m in matrices:
        only = jnp.where(diagonal, m, 0.0)
        across = lax.rsqrt(jnp.sum(only, axis=0, keepdims=True))
        down = lax.rsqrt(jnp.sum(only, axis=1, keepdims=True))
        scales.append((across, down))
        scaled.append((m * across) * down)
    one, two = scaled
    packed = sweep(jnp.where(low, one[:half], pltpu.roll(two[:half], half, 1)))
    corner = [jnp.where(low, packed, 0.0), jnp.where(low, pltpu.roll(packed, half, 1), 0.0)]
    upper, rest = [], []
    for m, each in zip(scaled, corner):
        over = jnp.where(low, 0.0, dot_high(each, m))
        over = jnp.concatenate([over, nothing], axis=0)
        upper.append(over)
        rest.append(m[half:] - dot_high(jnp.where(low, m[half:], 0.0), over))
    packed = sweep(jnp.where(low, pltpu.roll(rest[1], half, 1), rest[0]))
    final = [jnp.where(low, 0.0, packed), jnp.where(low, 0.0, pltpu.roll(packed, half, 1))]
    out = []
    for each, over, last, (across, down) in zip(corner, upper, final, scales):
        side = dot_high(over[:half], jnp.concatenate([nothing, last], axis=0))
        top = each + dot_last(side, over) - side
        bottom = last - dot_last(last, over)
        out.append((jnp.concatenate([top, bottom], axis=0) * across) * down)
    return out


def smooth_kernel(
    drive, gain, cov, observations, own, updated, moved, held, arrived,
):
    length, width = drive.shape
    panel = pltpu.make_async_copy(observations, held, arrived)
    panel.start()
    block = own.shape[0]
    place = pl.multiple_of(lax.axis_index("tm") * block, block)
    own[...] = drive[pl.ds(place, block), :]
    whole = drive[...]
    high, rest = halves(whole)
    factors = high.T
    time = lax.broadcasted_iota(jnp.int32, whole.shape, 0)
    kept = halves(jnp.where(time == length - 1, 0.0, whole))
    lag = halves(shift_rows(whole, 1))
    sums = jnp.dot(
        jnp.concatenate([factors, rest.T], axis=0),
        jnp.concatenate(kept + lag, axis=1),
        preferred_element_type=jnp.float32,
    )
    sums = sums[:width] + sums[width:]
    previous = sums[:, :width] + sums[:, width : 2 * width]
    lagged = sums[:, 2 * width : 3 * width] + sums[:, 3 * width :]
    final = whole[length - 8 :, :]
    final = jnp.where(lax.broadcasted_iota(jnp.int32, final.shape, 0) == 7, final, 0.0)
    total = previous + dot_first(final, final)
    total = total + length * cov[...]
    previous = previous + (length - 1) * cov[...]
    lagged = lagged + (length - 1) * dot_high(cov[...], gain[...].T)
    panel.wait()
    series = updated.shape[0]
    parts = [slice(start, min(start + 256, series)) for start in range(0, series, 256)]
    for part in parts:
        updated[part, :] = jnp.dot(
            factors, held[:, part], preferred_element_type=jnp.float32
        ).T
    total, previous = invert([total, previous])
    total = weights(total)
    for part in parts:
        updated[part, :] = times(updated[part, :], total)
    moved[...] = dot_high(lagged, previous)


def local(
    observations, loadings, noise_precision, transition, filter_cov, smoother_gain, smoothed_cov
):
    blocks = lax.axis_size("tm")
    planes = lax.axis_size("sr")
    width = transition.shape[0]
    length = observations.shape[0]
    steps_dev = length // blocks
    factors = gather(
        observations, loadings, noise_precision, transition, filter_cov, smoother_gain,
        blocks, planes,
    )
    vmem = pl.BlockSpec(memory_space=pltpu.VMEM)
    series = observations.shape[1]
    return pl.pallas_call(
        smooth_kernel,
        out_shape=[
            jax.ShapeDtypeStruct((steps_dev, width), jnp.float32),
            jax.ShapeDtypeStruct((series, width), jnp.float32),
            jax.ShapeDtypeStruct((width, width), jnp.float32),
        ],
        in_specs=[vmem] * 3 + [pl.BlockSpec(memory_space=pl.ANY)],
        out_specs=[vmem] * 3,
        scratch_shapes=[
            pltpu.VMEM((length, series), observations.dtype),
            pltpu.SemaphoreType.DMA,
        ],
        name="smooth",
    )(factors, smoother_gain, smoothed_cov, observations)


def solution(mesh):
    in_specs = (P(None, ("sr", "tm")), P(("sr", "tm"), None), P(("sr", "tm")), P(), P(), P(), P())
    out_specs = (P("tm", None), P(("sr", "tm"), None), P())
    return jax.shard_map(local, mesh=mesh, in_specs=in_specs, out_specs=out_specs, check_vma=False)
```

```python
import functools
import jax
import jax.numpy as jnp
from jax import lax
from jax.experimental import pallas as pl
from jax.experimental.pallas import tpu as pltpu
from jax.sharding import PartitionSpec as P

precise = lax.Precision.HIGHEST
MESH = pl.DeviceIdType.MESH
SLABS = 8
PIVOTS = 4
GRANT = 24 * 2**20


def dot_high(left, right):
    return jnp.dot(left, right, precision=precise, preferred_element_type=jnp.float32)


def dot_first(left, right):
    return lax.dot_general(
        left, right, (((0,), (0,)), ((), ())), precision=precise, preferred_element_type=jnp.float32
    )


def halves(value):
    high = value.astype(jnp.bfloat16)
    low = (value - high.astype(jnp.float32)).astype(jnp.bfloat16)
    return high, low


def weights(matrix):
    high, low = halves(matrix)
    side = jnp.concatenate([high, low], axis=1)
    return jnp.concatenate([side, side], axis=0)


def times(value, doubled):
    high, low = halves(value)
    width = value.shape[1]
    out = jnp.dot(
        jnp.concatenate([high, low], axis=1), doubled, preferred_element_type=jnp.float32
    )
    return out[:, :width] + out[:, width:]


def gather_kernel(
    blocks, planes, observations, loadings, precision_in, transition_in, filter_cov_in, gain_in,
    drive, panel, precision, transition, filter_cov, gain, small_done,
    near, far, out, out_info, rows_in, part, part_info, *scratch,
):
    chips = blocks // 2
    _, _, lows, rows, width = part.shape
    highs = planes // lows
    length, series = panel.shape
    share = part_info.shape[3]
    block = length // blocks
    steps = chips * lows
    tm = lax.axis_index("tm")
    sr = lax.axis_index("sr")
    core = lax.rem(tm, 2)
    chip = tm // 2
    other = 1 - core
    low = lax.rem(sr, lows)
    high = sr // lows
    partner = (2 * chip + other, sr)
    order = list(range(lows, steps)) + list(range(lows))[::-1]

    def chip_at(step):
        return lax.rem(chip + step // lows, chips)

    def low_at(step):
        return lax.rem(low + step % lows, lows)

    def member(step):
        return (2 * chip_at(step) + core, high * lows + low_at(step))

    def level(step):
        return (tm, lax.rem(high + step, highs) * lows + low)

    loads_done, panel_done = scratch[:2]
    given = (precision_in, transition_in, filter_cov_in, gain_in)
    kept = (precision, transition, filter_cov, gain)
    smalls = [
        pltpu.make_async_copy(source, target, small_done.at[at])
        for at, (source, target) in enumerate(zip(given, kept))
    ]
    for copy in smalls:
        copy.start()
    pieces = loads_done.shape[0]
    depth = series // pieces
    loads = []
    for at in range(pieces):
        here = slice(at * depth, (at + 1) * depth)
        loads.append(
            pltpu.make_async_copy(loadings.at[here, :], rows_in.at[here, :], loads_done.at[at])
        )
        loads[-1].start()
    tall = 2 * block
    panels = {}
    for step in list(range(1, chips)) + [0]:
        start = pl.multiple_of(lax.rem(chip + step, chips) * tall, tall)
        panels[step] = pltpu.make_async_copy(
            observations.at[pl.ds(start, tall), :],
            panel.at[pl.ds(start, tall), :],
            panel_done.at[step],
        )
        panels[step].start()

    barrier = pltpu.get_barrier_semaphore()
    pl.semaphore_signal(barrier, inc=1, device_id=partner, device_id_type=MESH)
    for step in range(1, steps):
        pl.semaphore_signal(barrier, inc=1, device_id=member(step), device_id_type=MESH)
    for step in range(1, highs):
        pl.semaphore_signal(barrier, inc=1, device_id=level(step), device_id_type=MESH)

    both = None
    weighted = []
    smalls[0].wait()
    for at in range(pieces):
        here = slice(at * depth, (at + 1) * depth)
        columns = [
            jnp.broadcast_to(precision[pl.ds(row, 1), :], (width, width)).T
            for row in range(at * depth // width, (at + 1) * depth // width)
        ]
        loads[at].wait()
        value = rows_in[here, :]
        scaled = value * jnp.concatenate(columns, axis=0)
        pair = halves(scaled)
        weighted.append(pair[0])
        left = jnp.concatenate(halves(value), axis=1)
        right = jnp.concatenate(pair, axis=1)
        each = lax.dot_general(
            left, right, (((0,), (0,)), ((), ())), preferred_element_type=jnp.float32
        )
        both = each if both is None else both + each
    weighted = jnp.concatenate(weighted, axis=0)
    both = both[:width] + both[width:]
    info = both[:, :width] + both[:, width:]
    for place in range(2 * steps):
        now = slice(place * share, (place + 1) * share)
        part_info[place // lows % 2, place // (2 * lows), place % lows] = info[now]
    pl.semaphore_wait(barrier, 1 + steps - 1 + highs - 1)

    class Stream:
        def __init__(self, part, out, pair_in, mine, cube_in, far_in, pair, across, far, back, last):
            self.part, self.out = part, out
            self.pair_in, self.mine, self.cube_in, self.far_in = pair_in, mine, cube_in, far_in
            self.pair, self.across, self.far, self.back, self.last = pair, across, far, back, last
            self.sent = []
            self.open = {}

        def send(self, key, source, target, semaphores, at, device):
            copy = pltpu.make_async_remote_copy(
                src_ref=source, dst_ref=target,
                send_sem=semaphores.at[0, at], recv_sem=semaphores.at[1, at],
                device_id=device, device_id_type=MESH,
            )
            copy.start()
            self.open[key] = copy
            self.sent.append(copy)

        def wait(self, key):
            self.open[key].wait_recv()

        def to_pair(self, step):
            source = self.part.at[other, chip_at(step), low_at(step)]
            self.send(("pair", step), source, self.pair_in.at[step], self.pair, step, partner)

        def to_cube(self, step):
            self.wait(("pair", step))
            self.mine[step] = self.part[core, chip_at(step), low_at(step)] + self.pair_in[step]
            if step > 0:
                self.send(
                    ("across", step), self.mine.at[step], self.cube_in.at[step],
                    self.across, step, member(step),
                )

        def to_far(self):
            total = self.mine[0]
            for step in order[:-1]:
                self.wait(("across", step))
                total = total + self.cube_in[step]
            self.far_in[high] = total
            for step in range(1, highs):
                self.send(
                    ("far", step), self.far_in.at[high], self.far_in.at[high],
                    self.far, step, level(step),
                )

        def to_back(self):
            for step in range(1, highs):
                self.wait(("far", step))
            total = self.far_in[0]
            for step in range(1, highs):
                total = total + self.far_in[step]
            here = self.out.at[core, chip, low]
            here[...] = total
            for step in order[:-1]:
                self.send(("back", step), here, here, self.back, step, member(step))
            self.send(("last", 0), here, here, self.last, 0, partner)

        def to_last(self, step):
            self.wait(("back", step))
            source = lax.rem(chip + chips - step // lows, chips)
            here = self.out.at[core, source, lax.rem(low + lows - step % lows, lows)]
            self.send(("last", step), here, here, self.last, step, partner)

    small = Stream(part_info, out_info, *scratch[2:11])
    large = Stream(part, out, *scratch[11:20])
    for step in order:
        small.to_pair(step)
    waiting = []
    for turn in list(range(1, chips)) + [0]:
        panels[turn].wait()
        source = lax.rem(chip + turn, chips)
        start = pl.multiple_of(source * tall, tall)
        proj = jnp.dot(
            panel[pl.ds(start, tall), :], weighted, preferred_element_type=jnp.float32
        )
        for at in range(2):
            for half in range(lows):
                now = slice(at * block + half * rows, at * block + (half + 1) * rows)
                part[at, source, half] = proj[now]
        fresh = [step for step in order if step // lows == turn]
        for step in fresh:
            large.to_pair(step)
        if turn == 1 % chips:
            for step in order:
                small.to_cube(step)
        for step in waiting:
            large.to_cube(step)
        waiting = fresh
    for step in waiting:
        large.to_cube(step)
    small.to_far()
    for copy in smalls[1:]:
        copy.wait()
    for _ in powers(gain[...].T, near.at[1], far.at[1]):
        pass
    cov_t = weights(filter_cov[...].T)
    coupled = weights(dot_high(gain[...], transition[...]).T)
    large.to_far()
    small.to_back()
    large.to_back()
    for step in order[:-1]:
        small.to_last(step)
    for step in order:
        small.wait(("last", step))
    places = [
        (at, turn, half) for turn in range(chips) for at in range(2) for half in range(lows)
    ]
    info = jnp.concatenate([out_info[place] for place in places], axis=0)
    closed = transition[...] - dot_high(filter_cov[...], dot_high(info, transition[...]))
    for _ in powers(closed.T, near.at[0], far.at[0]):
        pass

    def enter(at, step):
        source = lax.rem(chip + chips - step // lows, chips)
        half = lax.rem(low + lows - step % lows, lows)
        start = pl.multiple_of((2 * source + at) * block + half * rows, rows)
        drive[pl.ds(start, rows), :] = times(out[at, source, half], cov_t)

    enter(core, 0)
    for step in order[:-1]:
        large.to_last(step)
        enter(core, step)
    for step in [0] + order[:-1]:
        large.wait(("last", step))
        enter(other, step)
    count = length // SLABS
    slabs = [drive[pl.ds(at, count, stride=SLABS), :] for at in range(SLABS)]
    filtered = scan_slabs(slabs, near.at[0], far.at[0], False)
    final = lax.broadcasted_iota(jnp.int32, (count, width), 0) == count - 1
    back = [each - times(each, coupled) for each in filtered]
    back[-1] = jnp.where(final, filtered[-1], back[-1])
    smooth = scan_slabs(back, near.at[1], far.at[1], True)
    for at in range(SLABS):
        drive[pl.ds(at, count, stride=SLABS), :] = smooth[at]
    for stream in (small, large):
        for copy in stream.sent:
            copy.wait_send()


def stay(*arrays):
    return [pltpu.with_memory_space_constraint(array, pltpu.HBM) for array in arrays]


def gather(observations, loadings, noise_precision, transition, filter_cov, gain, blocks, planes):
    length, series = observations.shape
    width = loadings.shape[1]
    chips = blocks // 2
    lows = 2 if planes % 2 == 0 else 1
    highs = planes // lows
    rows = length // (blocks * lows)
    share = width // (blocks * lows)
    pieces = min(4, series // width)
    dma = pltpu.SemaphoreType.DMA
    vmem = pl.BlockSpec(memory_space=pltpu.VMEM)
    hbm = pl.BlockSpec(memory_space=pltpu.HBM)
    steps = chips * lows
    levels = (length // SLABS - 1).bit_length()

    def memory(*shape):
        return pltpu.VMEM(shape, jnp.float32)

    def stream(tall):
        return [memory(steps, tall, width)] * 3 + [memory(highs, tall, width)] + (
            [dma((2, steps))] * 2 + [dma((2, highs))] + [dma((2, steps))] * 2
        )

    shapes = [(2, chips, lows, tall, width) for tall in (rows, share)]
    return pl.pallas_call(
        functools.partial(gather_kernel, blocks, planes),
        out_shape=[
            pltpu.VMEM((length, width), jnp.float32),
            pltpu.VMEM((length, series), observations.dtype),
        ],
        in_specs=[hbm] * 6,
        out_specs=[vmem, vmem],
        scratch_shapes=[
            memory(series // width, width),
            memory(width, width),
            memory(width, width),
            memory(width, width),
            dma((4,)),
            pltpu.VMEM((2, SLABS - 1, 2 * width, 2 * width), jnp.bfloat16),
            pltpu.VMEM((2, levels, 2 * width, 2 * width), jnp.bfloat16),
            memory(*shapes[0]),
            memory(*shapes[1]),
            memory(series, width),
            memory(*shapes[0]),
            memory(*shapes[1]),
            dma((pieces,)),
            dma((chips,)),
        ]
        + stream(share)
        + stream(rows),
        compiler_params=pltpu.CompilerParams(
            collective_id=0, has_side_effects=True, vmem_limit_bytes=GRANT
        ),
        name="gather",
    )(
        *stay(
            observations, loadings, noise_precision.reshape(series // width, width),
            transition, filter_cov, gain,
        )
    )


def shift_rows(value, steps):
    length = value.shape[0]
    row = lax.broadcasted_iota(jnp.int32, value.shape, 0)
    moved = pltpu.roll(value, steps % length, 0)
    keep = row >= steps if steps > 0 else row < length + steps
    return jnp.where(keep, moved, 0.0)


def powers(matrix, low, high):
    made = [matrix]
    low[0] = weights(matrix)
    while len(made) < SLABS:
        fresh = [dot_high(made[-1], each) for each in made]
        for each in fresh:
            if len(made) < SLABS - 1:
                low[len(made)] = weights(each)
            made.append(each)
        yield
    square = made[-1]
    high[0] = weights(square)
    for level in range(1, high.shape[0]):
        square = dot_high(square, square)
        high[level] = weights(square)
        yield


def scan_slabs(slabs, low, high, reverse):
    order = list(range(SLABS))[::-1] if reverse else list(range(SLABS))
    sign = -1 if reverse else 1
    part = {order[0]: slabs[order[0]]}
    for before, now in zip(order, order[1:]):
        part[now] = slabs[now] + times(part[before], low[0])
    ends = part[order[-1]]
    for level in range(high.shape[0]):
        ends = ends + times(shift_rows(ends, sign * 2**level), high[level])
    carry = shift_rows(ends, sign)
    out = [None] * SLABS
    for place, now in enumerate(order[:-1]):
        out[now] = part[now] + times(carry, low[place])
    out[order[-1]] = ends
    return out


def inverse_two(a, b, c):
    scale = 1.0 / (a * c - b * b)
    return c * scale, -b * scale, a * scale


def inverse_four(p):
    e, f, g = inverse_two(p[0][0], p[0][1], p[1][1])
    u00 = e * p[0][2] + f * p[1][2]
    u01 = e * p[0][3] + f * p[1][3]
    u10 = f * p[0][2] + g * p[1][2]
    u11 = f * p[0][3] + g * p[1][3]
    s00 = p[2][2] - (p[0][2] * u00 + p[1][2] * u10)
    s01 = p[2][3] - (p[0][2] * u01 + p[1][2] * u11)
    s11 = p[3][3] - (p[0][3] * u01 + p[1][3] * u11)
    t00, t01, t11 = inverse_two(s00, s01, s11)
    v00 = u00 * t00 + u01 * t01
    v01 = u00 * t01 + u01 * t11
    v10 = u10 * t00 + u11 * t01
    v11 = u10 * t01 + u11 * t11
    a00 = e + (v00 * u00 + v01 * u01)
    a01 = f + (v00 * u10 + v01 * u11)
    a11 = g + (v10 * u10 + v11 * u11)
    return [
        [a00, a01, -v00, -v01],
        [a01, a11, -v10, -v11],
        [-v00, -v10, t00, t01],
        [-v01, -v11, t01, t11],
    ]


def dot_last(left, right):
    return lax.dot_general(left, right, (((1,), (1,)), ((), ())), precision=precise, preferred_element_type=jnp.float32)


def pick(value, lane, half, at):
    index = jnp.where(lane >= half, half + at, at)
    return jnp.take_along_axis(value, index, axis=1, mode="promise_in_bounds")

def sweep(packed):
    half, size = packed.shape
    lane = lax.broadcasted_iota(jnp.int32, (8, size), 1)
    inner = jnp.where(lane >= half, lane - half, lane)
    sub = lax.broadcasted_iota(jnp.int32, (8, size), 0)
    groups = half // 8
    value = [packed[8 * g : 8 * g + 8] for g in range(groups)]

    def spread(tile, at):
        return jnp.broadcast_to(tile[at : at + 1, :], (8, size))

    first = [pick(value[0], lane, half, j) for j in range(PIVOTS)]
    block = [[spread(first[max(i, j)], min(i, j)) for j in range(PIVOTS)] for i in range(PIVOTS)]
    for k in range(0, half, PIVOTS):
        group, place = divmod(k, 8)
        solved = inverse_four(block)
        order = list(range(groups))
        following = k + PIVOTS
        if following < half:
            ahead, spot = divmod(following, 8)
            order.remove(ahead)
            order.insert(0, ahead)
        columns = [None] * groups
        for g in order:
            columns[g] = [pick(value[g], lane, half, k + j) for j in range(PIVOTS)]
            if g == order[0] and following < half:
                coming = [pick(value[g], lane, half, following + j) for j in range(PIVOTS)]
        if following < half:
            cross = [[spread(columns[ahead][j], spot + i) for j in range(PIVOTS)] for i in range(PIVOTS)]
            moved = [[sum(solved[i][j] * cross[b][j] for j in range(PIVOTS)) for b in range(PIVOTS)] for i in range(PIVOTS)]
            block = [[None] * PIVOTS for _ in range(PIVOTS)]
            for a in range(PIVOTS):
                for b in range(a, PIVOTS):
                    take = sum(cross[a][i] * moved[i][b] for i in range(PIVOTS))
                    block[a][b] = block[b][a] = spread(coming[b], spot + a) - take
        here = (inner >= k) & (inner < k + PIVOTS)
        rows = []
        for i in range(PIVOTS):
            row = jnp.where(here, 0.0, spread(value[group], place + i))
            rows.append(jnp.where(inner == k + i, 1.0, row))
        fresh = [sum(solved[i][j] * rows[j] for j in range(PIVOTS)) for i in range(PIVOTS)]
        updated = [None] * groups
        for g in order:
            take = sum(columns[g][i] * fresh[i] for i in range(PIVOTS))
            updated[g] = jnp.where(here, 0.0, value[g]) - take
            if g == group:
                for i in range(PIVOTS):
                    updated[g] = jnp.where(sub == place + i, fresh[i], updated[g])
        value = updated
    return jnp.concatenate(value, axis=0)


def invert(matrices):
    size = matrices[0].shape[0]
    half = size // 2
    row_at = lax.broadcasted_iota(jnp.int32, (size, size), 0)
    lane_at = lax.broadcasted_iota(jnp.int32, (size, size), 1)
    low = lax.broadcasted_iota(jnp.int32, (half, size), 1) < half
    nothing = jnp.zeros((half, size), jnp.float32)
    diagonal = row_at == lane_at
    scales, scaled = [], []
    for m in matrices:
        only = jnp.where(diagonal, m, 0.0)
        across = lax.rsqrt(jnp.sum(only, axis=0, keepdims=True))
        down = lax.rsqrt(jnp.sum(only, axis=1, keepdims=True))
        scales.append((across, down))
        scaled.append((m * across) * down)
    one, two = scaled
    packed = sweep(jnp.where(low, one[:half], pltpu.roll(two[:half], half, 1)))
    corner = [jnp.where(low, packed, 0.0), jnp.where(low, pltpu.roll(packed, half, 1), 0.0)]
    upper, rest = [], []
    for m, each in zip(scaled, corner):
        over = jnp.where(low, 0.0, dot_high(each, m))
        over = jnp.concatenate([over, nothing], axis=0)
        upper.append(over)
        rest.append(m[half:] - dot_high(jnp.where(low, m[half:], 0.0), over))
    packed = sweep(jnp.where(low, pltpu.roll(rest[1], half, 1), rest[0]))
    final = [jnp.where(low, 0.0, packed), jnp.where(low, 0.0, pltpu.roll(packed, half, 1))]
    out = []
    for each, over, last, (across, down) in zip(corner, upper, final, scales):
        side = dot_high(over[:half], jnp.concatenate([nothing, last], axis=0))
        top = each + dot_last(side, over) - side
        bottom = last - dot_last(last, over)
        out.append((jnp.concatenate([top, bottom], axis=0) * across) * down)
    return out


def smooth_kernel(
    drive, held, gain_in, cov_in, own, updated, moved_out, gain, cov, staged, moved,
    small_done, own_done, moved_done, part_done,
):
    length, width = drive.shape
    smalls = [
        pltpu.make_async_copy(gain_in, gain, small_done.at[0]),
        pltpu.make_async_copy(cov_in, cov, small_done.at[1]),
    ]
    for copy in smalls:
        copy.start()
    block = own.shape[0]
    place = pl.multiple_of(lax.axis_index("tm") * block, block)
    owned = pltpu.make_async_copy(drive.at[pl.ds(place, block), :], own, own_done)
    owned.start()
    whole = drive[...]
    high, rest = halves(whole)
    factors = high.T
    time = lax.broadcasted_iota(jnp.int32, whole.shape, 0)
    kept = halves(jnp.where(time == length - 1, 0.0, whole))
    lag = halves(shift_rows(whole, 1))
    sums = jnp.dot(
        jnp.concatenate([factors, rest.T], axis=0),
        jnp.concatenate(kept + lag, axis=1),
        preferred_element_type=jnp.float32,
    )
    sums = sums[:width] + sums[width:]
    previous = sums[:, :width] + sums[:, width : 2 * width]
    lagged = sums[:, 2 * width : 3 * width] + sums[:, 3 * width :]
    for copy in smalls:
        copy.wait()
    final = whole[length - 8 :, :]
    final = jnp.where(lax.broadcasted_iota(jnp.int32, final.shape, 0) == 7, final, 0.0)
    total = previous + dot_first(final, final)
    total = total + length * cov[...]
    previous = previous + (length - 1) * cov[...]
    lagged = lagged + (length - 1) * dot_high(cov[...], gain[...].T)
    series = held.shape[1]
    parts = [slice(start, min(start + 256, series)) for start in range(0, series, 256)]
    for part in parts:
        staged[part, :] = jnp.dot(
            factors, held[:, part], preferred_element_type=jnp.float32
        ).T
    total, previous = invert([total, previous])
    total = weights(total)
    moved[...] = dot_high(lagged, previous)
    writes = [owned, pltpu.make_async_copy(moved, moved_out, moved_done)]
    writes[-1].start()
    for at, part in enumerate(parts):
        staged[part, :] = times(staged[part, :], total)
        writes.append(
            pltpu.make_async_copy(staged.at[part, :], updated.at[part, :], part_done.at[at])
        )
        writes[-1].start()
    for copy in writes:
        copy.wait()


def local(
    observations, loadings, noise_precision, transition, filter_cov, smoother_gain, smoothed_cov
):
    blocks = lax.axis_size("tm")
    planes = lax.axis_size("sr")
    width = transition.shape[0]
    length = observations.shape[0]
    steps_dev = length // blocks
    factors, panel = gather(
        observations, loadings, noise_precision, transition, filter_cov, smoother_gain,
        blocks, planes,
    )
    vmem = pl.BlockSpec(memory_space=pltpu.VMEM)
    series = observations.shape[1]
    return pl.pallas_call(
        smooth_kernel,
        out_shape=[
            jax.ShapeDtypeStruct((steps_dev, width), jnp.float32),
            jax.ShapeDtypeStruct((series, width), jnp.float32),
            jax.ShapeDtypeStruct((width, width), jnp.float32),
        ],
        in_specs=[vmem] * 2 + [pl.BlockSpec(memory_space=pltpu.HBM)] * 2,
        out_specs=[pl.BlockSpec(memory_space=pltpu.HBM)] * 3,
        scratch_shapes=[
            pltpu.VMEM((width, width), jnp.float32),
            pltpu.VMEM((width, width), jnp.float32),
            pltpu.VMEM((series, width), jnp.float32),
            pltpu.VMEM((width, width), jnp.float32),
            pltpu.SemaphoreType.DMA((2,)),
            pltpu.SemaphoreType.DMA,
            pltpu.SemaphoreType.DMA,
            pltpu.SemaphoreType.DMA((pl.cdiv(series, 256),)),
        ],
        compiler_params=pltpu.CompilerParams(vmem_limit_bytes=GRANT),
        name="smooth",
    )(factors, panel, *stay(smoother_gain, smoothed_cov))


def solution(mesh):
    in_specs = (P(None, ("sr", "tm")), P(("sr", "tm"), None), P(("sr", "tm")), P(), P(), P(), P())
    out_specs = (P("tm", None), P(("sr", "tm"), None), P())
    return jax.shard_map(local, mesh=mesh, in_specs=in_specs, out_specs=out_specs, check_vma=False)
```

```python
import functools
import jax
import jax.numpy as jnp
from jax import lax
from jax.experimental import pallas as pl
from jax.experimental.pallas import tpu as pltpu
from jax.sharding import PartitionSpec as P

precise = lax.Precision.HIGHEST
MESH = pl.DeviceIdType.MESH
SLABS = 8
PIVOTS = 4
GRANT = 24 * 2**20


def dot_high(left, right):
    return jnp.dot(left, right, precision=precise, preferred_element_type=jnp.float32)


def dot_first(left, right):
    return lax.dot_general(
        left, right, (((0,), (0,)), ((), ())), precision=precise, preferred_element_type=jnp.float32
    )


def halves(value):
    high = value.astype(jnp.bfloat16)
    low = (value - high.astype(jnp.float32)).astype(jnp.bfloat16)
    return high, low


def weights(matrix):
    high, low = halves(matrix)
    side = jnp.concatenate([high, low], axis=1)
    return jnp.concatenate([side, side], axis=0)


def times(value, doubled):
    high, low = halves(value)
    width = value.shape[1]
    out = jnp.dot(
        jnp.concatenate([high, low], axis=1), doubled, preferred_element_type=jnp.float32
    )
    return out[:, :width] + out[:, width:]


def gather_kernel(
    blocks, planes, observations, loadings, precision_in, transition_in, filter_cov_in, gain_in,
    drive, panel, precision, transition, filter_cov, gain, small_done,
    tables, out, out_info, rows_in, part, part_info, *scratch,
):
    chips = blocks // 2
    _, _, lows, rows, width = part.shape
    highs = planes // lows
    length, series = panel.shape
    share = part_info.shape[3]
    block = length // blocks
    steps = chips * lows
    tm = lax.axis_index("tm")
    sr = lax.axis_index("sr")
    core = lax.rem(tm, 2)
    chip = tm // 2
    other = 1 - core
    low = lax.rem(sr, lows)
    high = sr // lows
    partner = (2 * chip + other, sr)
    turns = sorted(range(1, chips), key=lambda turn: -turn.bit_count()) + [0]
    order = [turn * lows + half for turn in turns for half in range(lows)[::-1]]
    nearest = order[:-1][::-1]

    def across_to(turn):
        place = 0
        for bit in range((chips - 1).bit_length()):
            mine = lax.rem(chip // 2**bit + turn // 2**bit, 2)
            place = place + mine * 2**bit
        return place

    def across_from(turn):
        return across_to(turn)

    if chips & (chips - 1):

        def across_to(turn):
            return lax.rem(chip + turn, chips)

        def across_from(turn):
            return lax.rem(chip + chips - turn, chips)

    def chip_at(step):
        return across_to(step // lows)

    def low_at(step):
        return lax.rem(low + step % lows, lows)

    def member(step):
        return (2 * chip_at(step) + core, high * lows + low_at(step))

    def level(step):
        return (tm, lax.rem(high + step, highs) * lows + low)

    loads_done, panel_done = scratch[:2]
    given = (precision_in, transition_in, filter_cov_in, gain_in)
    kept = (precision, transition, filter_cov, gain)
    smalls = [
        pltpu.make_async_copy(source, target, small_done.at[at])
        for at, (source, target) in enumerate(zip(given, kept))
    ]
    for copy in smalls:
        copy.start()
    pieces = loads_done.shape[0]
    depth = series // pieces
    loads = []
    for at in range(pieces):
        here = slice(at * depth, (at + 1) * depth)
        loads.append(
            pltpu.make_async_copy(loadings.at[here, :], rows_in.at[here, :], loads_done.at[at])
        )
        loads[-1].start()
    tall = 2 * block
    panels = {}
    for step in turns:
        start = pl.multiple_of(across_to(step) * tall, tall)
        panels[step] = pltpu.make_async_copy(
            observations.at[pl.ds(start, tall), :],
            panel.at[pl.ds(start, tall), :],
            panel_done.at[step],
        )
        panels[step].start()

    barrier = pltpu.get_barrier_semaphore()
    pl.semaphore_signal(barrier, inc=1, device_id=partner, device_id_type=MESH)
    for step in range(1, steps):
        pl.semaphore_signal(barrier, inc=1, device_id=member(step), device_id_type=MESH)
    for step in range(1, highs):
        pl.semaphore_signal(barrier, inc=1, device_id=level(step), device_id_type=MESH)

    both = None
    weighted = []
    smalls[0].wait()
    for at in range(pieces):
        here = slice(at * depth, (at + 1) * depth)
        columns = [
            jnp.broadcast_to(precision[pl.ds(row, 1), :], (width, width)).T
            for row in range(at * depth // width, (at + 1) * depth // width)
        ]
        loads[at].wait()
        value = rows_in[here, :]
        scaled = value * jnp.concatenate(columns, axis=0)
        pair = halves(scaled)
        weighted.append(pair[0])
        left = jnp.concatenate(halves(value), axis=1)
        right = jnp.concatenate(pair, axis=1)
        each = lax.dot_general(
            left, right, (((0,), (0,)), ((), ())), preferred_element_type=jnp.float32
        )
        both = each if both is None else both + each
    weighted = jnp.concatenate(weighted, axis=0)
    both = both[:width] + both[width:]
    info = both[:, :width] + both[:, width:]
    for place in range(2 * steps):
        now = slice(place * share, (place + 1) * share)
        part_info[place // lows % 2, place // (2 * lows), place % lows] = info[now]
    pl.semaphore_wait(barrier, 1 + steps - 1 + highs - 1)

    class Stream:
        def __init__(self, part, out, pair_in, mine, cube_in, far_in, pair, across, far, back, last):
            self.part, self.out = part, out
            self.pair_in, self.mine, self.cube_in, self.far_in = pair_in, mine, cube_in, far_in
            self.pair, self.across, self.far, self.back, self.last = pair, across, far, back, last
            self.sent = []
            self.open = {}

        def send(self, key, source, target, semaphores, at, device):
            copy = pltpu.make_async_remote_copy(
                src_ref=source, dst_ref=target,
                send_sem=semaphores.at[0, at], recv_sem=semaphores.at[1, at],
                device_id=device, device_id_type=MESH,
            )
            copy.start()
            self.open[key] = copy
            self.sent.append(copy)

        def wait(self, key):
            self.open[key].wait_recv()

        def to_pair(self, step):
            source = self.part.at[other, chip_at(step), low_at(step)]
            self.send(("pair", step), source, self.pair_in.at[step], self.pair, step, partner)

        def to_cube(self, step):
            self.wait(("pair", step))
            self.mine[step] = self.part[core, chip_at(step), low_at(step)] + self.pair_in[step]
            if step > 0:
                self.send(
                    ("across", step), self.mine.at[step], self.cube_in.at[step],
                    self.across, step, member(step),
                )

        def to_far(self):
            total = self.mine[0]
            for step in nearest:
                self.wait(("across", step))
                total = total + self.cube_in[step]
            self.far_in[high] = total
            for step in range(1, highs):
                self.send(
                    ("far", step), self.far_in.at[high], self.far_in.at[high],
                    self.far, step, level(step),
                )

        def to_back(self):
            for step in range(1, highs):
                self.wait(("far", step))
            total = self.far_in[0]
            for step in range(1, highs):
                total = total + self.far_in[step]
            here = self.out.at[core, chip, low]
            here[...] = total
            for step in order[:-1]:
                self.send(("back", step), here, here, self.back, step, member(step))
            self.send(("last", 0), here, here, self.last, 0, partner)

        def to_last(self, step):
            self.wait(("back", step))
            source = across_from(step // lows)
            here = self.out.at[core, source, lax.rem(low + lows - step % lows, lows)]
            self.send(("last", step), here, here, self.last, step, partner)

    small = Stream(part_info, out_info, *scratch[2:11])
    large = Stream(part, out, *scratch[11:20])
    for step in order:
        small.to_pair(step)
    waiting = []
    for turn in turns:
        panels[turn].wait()
        source = across_to(turn)
        start = pl.multiple_of(source * tall, tall)
        proj = jnp.dot(
            panel[pl.ds(start, tall), :], weighted, preferred_element_type=jnp.float32
        )
        for at in range(2):
            for half in range(lows):
                now = slice(at * block + half * rows, at * block + (half + 1) * rows)
                part[at, source, half] = proj[now]
        fresh = [step for step in order if step // lows == turn]
        for step in fresh:
            large.to_pair(step)
        if turn == turns[0]:
            for step in order:
                small.to_cube(step)
        for step in waiting:
            large.to_cube(step)
        waiting = fresh
    for step in waiting:
        large.to_cube(step)
    small.to_far()
    count = length // SLABS
    for copy in smalls[1:]:
        copy.wait()
    powers(gain[...].T, tables.at[1], count)
    cov_t = weights(filter_cov[...].T)
    coupled = weights(dot_high(gain[...], transition[...]).T)
    large.to_far()
    small.to_back()
    large.to_back()
    for step in nearest:
        small.to_last(step)
    for step in [0] + nearest:
        small.wait(("last", step))
    places = [
        (at, turn, half) for turn in range(chips) for at in range(2) for half in range(lows)
    ]
    info = jnp.concatenate([out_info[place] for place in places], axis=0)
    closed = transition[...] - dot_high(filter_cov[...], dot_high(info, transition[...]))
    powers(closed.T, tables.at[0], count)
    for step in nearest:
        large.to_last(step)

    def enter(at):
        tall = chips * lows * rows
        given = out[at].reshape(tall, width)
        entered = times(given, cov_t)
        for turn in range(chips):
            for half in range(lows):
                start = pl.multiple_of((2 * turn + at) * block + half * rows, rows)
                now = (turn * lows + half) * rows
                drive[pl.ds(start, rows), :] = entered[now : now + rows]

    enter(core)
    for step in [0] + nearest:
        large.wait(("last", step))
    enter(other)
    slabs = [drive[pl.ds(at, count, stride=SLABS), :] for at in range(SLABS)]
    filtered = scan_slabs(slabs, tables.at[0], False)
    final = lax.broadcasted_iota(jnp.int32, (count, width), 0) == count - 1
    back = [each - times(each, coupled) for each in filtered]
    back[-1] = jnp.where(final, filtered[-1], back[-1])
    smooth = scan_slabs(back, tables.at[1], True)
    for at in range(SLABS):
        drive[pl.ds(at, count, stride=SLABS), :] = smooth[at]
    for stream in (small, large):
        for copy in stream.sent:
            copy.wait_send()


def stay(*arrays):
    return [pltpu.with_memory_space_constraint(array, pltpu.HBM) for array in arrays]


def gather(observations, loadings, noise_precision, transition, filter_cov, gain, blocks, planes):
    length, series = observations.shape
    width = loadings.shape[1]
    chips = blocks // 2
    lows = 2 if planes % 2 == 0 else 1
    highs = planes // lows
    rows = length // (blocks * lows)
    share = width // (blocks * lows)
    pieces = min(4, series // width)
    dma = pltpu.SemaphoreType.DMA
    vmem = pl.BlockSpec(memory_space=pltpu.VMEM)
    hbm = pl.BlockSpec(memory_space=pltpu.HBM)
    steps = chips * lows
    entries = sum(radix - 1 for radix in [SLABS] + radices(length // SLABS))

    def memory(*shape):
        return pltpu.VMEM(shape, jnp.float32)

    def stream(tall):
        return [memory(steps, tall, width)] * 3 + [memory(highs, tall, width)] + (
            [dma((2, steps))] * 2 + [dma((2, highs))] + [dma((2, steps))] * 2
        )

    shapes = [(2, chips, lows, tall, width) for tall in (rows, share)]
    return pl.pallas_call(
        functools.partial(gather_kernel, blocks, planes),
        out_shape=[
            pltpu.VMEM((length, width), jnp.float32),
            pltpu.VMEM((length, series), observations.dtype),
        ],
        in_specs=[hbm] * 6,
        out_specs=[vmem, vmem],
        scratch_shapes=[
            memory(series // width, width),
            memory(width, width),
            memory(width, width),
            memory(width, width),
            dma((4,)),
            pltpu.VMEM((2, entries, 2 * width, 2 * width), jnp.bfloat16),
            memory(*shapes[0]),
            memory(*shapes[1]),
            memory(series, width),
            memory(*shapes[0]),
            memory(*shapes[1]),
            dma((pieces,)),
            dma((chips,)),
        ]
        + stream(share)
        + stream(rows),
        compiler_params=pltpu.CompilerParams(
            collective_id=0, has_side_effects=True, vmem_limit_bytes=GRANT
        ),
        name="gather",
    )(
        *stay(
            observations, loadings, noise_precision.reshape(series // width, width),
            transition, filter_cov, gain,
        )
    )


def shift_rows(value, steps):
    length = value.shape[0]
    row = lax.broadcasted_iota(jnp.int32, value.shape, 0)
    moved = pltpu.roll(value, steps % length, 0)
    keep = row >= steps if steps > 0 else row < length + steps
    return jnp.where(keep, moved, 0.0)


def radices(count):
    bits = (count - 1).bit_length()
    parts = -(-bits // 3)
    return [2 ** (bits * (at + 1) // parts - bits * at // parts) for at in range(parts)][::-1]


def powers(matrix, table, count):
    levels = [SLABS] + radices(count)
    base, start = matrix, 0
    for at, radix in enumerate(levels):
        made = [base]
        top = radix if at + 1 < len(levels) else radix - 1
        table[start] = weights(base)
        while len(made) < top:
            fresh = [dot_high(made[-1], each) for each in made][: top - len(made)]
            for each in fresh:
                if len(made) < radix - 1:
                    table[start + len(made)] = weights(each)
                made.append(each)
        base = made[-1]
        start += radix - 1


def times_many(values, table, start):
    width = values[0].shape[1]
    left = jnp.concatenate([part for value in values for part in halves(value)], axis=1)
    right = table[start : start + len(values)].reshape(2 * width * len(values), 2 * width)
    out = jnp.dot(left, right, preferred_element_type=jnp.float32)
    return out[:, :width] + out[:, width:]


def scan_slabs(slabs, table, reverse):
    order = list(range(SLABS))[::-1] if reverse else list(range(SLABS))
    sign = -1 if reverse else 1
    part = [slabs[now] for now in order]
    ends = part.pop()
    ends = ends + times_many(part[::-1], table, 0)
    start, stride = SLABS - 1, 1
    for radix in radices(ends.shape[0]):
        moved = [shift_rows(ends, sign * stride * at) for at in range(1, radix)]
        ends = ends + times_many(moved, table, start)
        start += radix - 1
        stride *= radix
    size = 1
    while size < SLABS:
        for first in range(size, SLABS - 1, 2 * size):
            for offset in range(min(size, SLABS - 1 - first)):
                add = times(part[first - 1], table[offset])
                part[first + offset] = part[first + offset] + add
        size *= 2
    carry = shift_rows(ends, sign)
    out = [None] * SLABS
    for place, now in enumerate(order[:-1]):
        out[now] = part[place] + times(carry, table[place])
    out[order[-1]] = ends
    return out


def inverse_two(a, b, c):
    scale = 1.0 / (a * c - b * b)
    return c * scale, -b * scale, a * scale


def inverse_four(p):
    e, f, g = inverse_two(p[0][0], p[0][1], p[1][1])
    u00 = e * p[0][2] + f * p[1][2]
    u01 = e * p[0][3] + f * p[1][3]
    u10 = f * p[0][2] + g * p[1][2]
    u11 = f * p[0][3] + g * p[1][3]
    s00 = p[2][2] - (p[0][2] * u00 + p[1][2] * u10)
    s01 = p[2][3] - (p[0][2] * u01 + p[1][2] * u11)
    s11 = p[3][3] - (p[0][3] * u01 + p[1][3] * u11)
    t00, t01, t11 = inverse_two(s00, s01, s11)
    v00 = u00 * t00 + u01 * t01
    v01 = u00 * t01 + u01 * t11
    v10 = u10 * t00 + u11 * t01
    v11 = u10 * t01 + u11 * t11
    a00 = e + (v00 * u00 + v01 * u01)
    a01 = f + (v00 * u10 + v01 * u11)
    a11 = g + (v10 * u10 + v11 * u11)
    return [
        [a00, a01, -v00, -v01],
        [a01, a11, -v10, -v11],
        [-v00, -v10, t00, t01],
        [-v01, -v11, t01, t11],
    ]


def dot_last(left, right):
    return lax.dot_general(left, right, (((1,), (1,)), ((), ())), precision=precise, preferred_element_type=jnp.float32)


def pick(value, lane, half, at):
    index = jnp.where(lane >= half, half + at, at)
    return jnp.take_along_axis(value, index, axis=1, mode="promise_in_bounds")

def sweep(packed):
    half, size = packed.shape
    lane = lax.broadcasted_iota(jnp.int32, (8, size), 1)
    inner = jnp.where(lane >= half, lane - half, lane)
    sub = lax.broadcasted_iota(jnp.int32, (8, size), 0)
    groups = half // 8
    value = [packed[8 * g : 8 * g + 8] for g in range(groups)]

    def spread(tile, at):
        return jnp.broadcast_to(tile[at : at + 1, :], (8, size))

    first = [pick(value[0], lane, half, j) for j in range(PIVOTS)]
    block = [[spread(first[max(i, j)], min(i, j)) for j in range(PIVOTS)] for i in range(PIVOTS)]
    for k in range(0, half, PIVOTS):
        group, place = divmod(k, 8)
        solved = inverse_four(block)
        order = list(range(groups))
        following = k + PIVOTS
        if following < half:
            ahead, spot = divmod(following, 8)
            order.remove(ahead)
            order.insert(0, ahead)
        columns = [None] * groups
        for g in order:
            columns[g] = [pick(value[g], lane, half, k + j) for j in range(PIVOTS)]
            if g == order[0] and following < half:
                coming = [pick(value[g], lane, half, following + j) for j in range(PIVOTS)]
        if following < half:
            cross = [[spread(columns[ahead][j], spot + i) for j in range(PIVOTS)] for i in range(PIVOTS)]
            moved = [[sum(solved[i][j] * cross[b][j] for j in range(PIVOTS)) for b in range(PIVOTS)] for i in range(PIVOTS)]
            block = [[None] * PIVOTS for _ in range(PIVOTS)]
            for a in range(PIVOTS):
                for b in range(a, PIVOTS):
                    take = sum(cross[a][i] * moved[i][b] for i in range(PIVOTS))
                    block[a][b] = block[b][a] = spread(coming[b], spot + a) - take
        here = (inner >= k) & (inner < k + PIVOTS)
        rows = []
        for i in range(PIVOTS):
            row = jnp.where(here, 0.0, spread(value[group], place + i))
            rows.append(jnp.where(inner == k + i, 1.0, row))
        fresh = [sum(solved[i][j] * rows[j] for j in range(PIVOTS)) for i in range(PIVOTS)]
        updated = [None] * groups
        for g in order:
            take = sum(columns[g][i] * fresh[i] for i in range(PIVOTS))
            updated[g] = jnp.where(here, 0.0, value[g]) - take
            if g == group:
                for i in range(PIVOTS):
                    updated[g] = jnp.where(sub == place + i, fresh[i], updated[g])
        value = updated
    return jnp.concatenate(value, axis=0)


def invert(matrices):
    size = matrices[0].shape[0]
    half = size // 2
    row_at = lax.broadcasted_iota(jnp.int32, (size, size), 0)
    lane_at = lax.broadcasted_iota(jnp.int32, (size, size), 1)
    low = lax.broadcasted_iota(jnp.int32, (half, size), 1) < half
    nothing = jnp.zeros((half, size), jnp.float32)
    diagonal = row_at == lane_at
    scales, scaled = [], []
    for m in matrices:
        only = jnp.where(diagonal, m, 0.0)
        across = lax.rsqrt(jnp.sum(only, axis=0, keepdims=True))
        down = lax.rsqrt(jnp.sum(only, axis=1, keepdims=True))
        scales.append((across, down))
        scaled.append((m * across) * down)
    one, two = scaled
    packed = sweep(jnp.where(low, one[:half], pltpu.roll(two[:half], half, 1)))
    corner = [jnp.where(low, packed, 0.0), jnp.where(low, pltpu.roll(packed, half, 1), 0.0)]
    upper, rest = [], []
    for m, each in zip(scaled, corner):
        over = jnp.where(low, 0.0, dot_high(each, m))
        over = jnp.concatenate([over, nothing], axis=0)
        upper.append(over)
        rest.append(m[half:] - dot_high(jnp.where(low, m[half:], 0.0), over))
    packed = sweep(jnp.where(low, pltpu.roll(rest[1], half, 1), rest[0]))
    final = [jnp.where(low, 0.0, packed), jnp.where(low, 0.0, pltpu.roll(packed, half, 1))]
    out = []
    for each, over, last, (across, down) in zip(corner, upper, final, scales):
        side = dot_high(over[:half], jnp.concatenate([nothing, last], axis=0))
        top = each + dot_last(side, over) - side
        bottom = last - dot_last(last, over)
        out.append((jnp.concatenate([top, bottom], axis=0) * across) * down)
    return out


def smooth_kernel(
    drive, held, gain_in, cov_in, own, updated, moved_out, gain, cov, staged, moved,
    small_done, own_done, moved_done, part_done,
):
    length, width = drive.shape
    smalls = [
        pltpu.make_async_copy(gain_in, gain, small_done.at[0]),
        pltpu.make_async_copy(cov_in, cov, small_done.at[1]),
    ]
    for copy in smalls:
        copy.start()
    block = own.shape[0]
    place = pl.multiple_of(lax.axis_index("tm") * block, block)
    owned = pltpu.make_async_copy(drive.at[pl.ds(place, block), :], own, own_done)
    owned.start()
    whole = drive[...]
    high, rest = halves(whole)
    factors = high.T
    time = lax.broadcasted_iota(jnp.int32, whole.shape, 0)
    kept = halves(jnp.where(time == length - 1, 0.0, whole))
    lag = halves(shift_rows(whole, 1))
    sums = jnp.dot(
        jnp.concatenate([factors, rest.T], axis=0),
        jnp.concatenate(kept + lag, axis=1),
        preferred_element_type=jnp.float32,
    )
    sums = sums[:width] + sums[width:]
    previous = sums[:, :width] + sums[:, width : 2 * width]
    lagged = sums[:, 2 * width : 3 * width] + sums[:, 3 * width :]
    for copy in smalls:
        copy.wait()
    final = whole[length - 8 :, :]
    final = jnp.where(lax.broadcasted_iota(jnp.int32, final.shape, 0) == 7, final, 0.0)
    total = previous + dot_first(final, final)
    total = total + length * cov[...]
    previous = previous + (length - 1) * cov[...]
    lagged = lagged + (length - 1) * dot_high(cov[...], gain[...].T)
    series = held.shape[1]
    parts = [slice(start, min(start + 256, series)) for start in range(0, series, 256)]
    for part in parts:
        staged[part, :] = jnp.dot(
            factors, held[:, part], preferred_element_type=jnp.float32
        ).T
    total, previous = invert([total, previous])
    total = weights(total)
    moved[...] = dot_high(lagged, previous)
    writes = [owned, pltpu.make_async_copy(moved, moved_out, moved_done)]
    writes[-1].start()
    for at, part in enumerate(parts):
        staged[part, :] = times(staged[part, :], total)
        writes.append(
            pltpu.make_async_copy(staged.at[part, :], updated.at[part, :], part_done.at[at])
        )
        writes[-1].start()
    for copy in writes:
        copy.wait()


def local(
    observations, loadings, noise_precision, transition, filter_cov, smoother_gain, smoothed_cov
):
    blocks = lax.axis_size("tm")
    planes = lax.axis_size("sr")
    width = transition.shape[0]
    length = observations.shape[0]
    steps_dev = length // blocks
    factors, panel = gather(
        observations, loadings, noise_precision, transition, filter_cov, smoother_gain,
        blocks, planes,
    )
    vmem = pl.BlockSpec(memory_space=pltpu.VMEM)
    series = observations.shape[1]
    return pl.pallas_call(
        smooth_kernel,
        out_shape=[
            jax.ShapeDtypeStruct((steps_dev, width), jnp.float32),
            jax.ShapeDtypeStruct((series, width), jnp.float32),
            jax.ShapeDtypeStruct((width, width), jnp.float32),
        ],
        in_specs=[vmem] * 2 + [pl.BlockSpec(memory_space=pltpu.HBM)] * 2,
        out_specs=[pl.BlockSpec(memory_space=pltpu.HBM)] * 3,
        scratch_shapes=[
            pltpu.VMEM((width, width), jnp.float32),
            pltpu.VMEM((width, width), jnp.float32),
            pltpu.VMEM((series, width), jnp.float32),
            pltpu.VMEM((width, width), jnp.float32),
            pltpu.SemaphoreType.DMA((2,)),
            pltpu.SemaphoreType.DMA,
            pltpu.SemaphoreType.DMA,
            pltpu.SemaphoreType.DMA((pl.cdiv(series, 256),)),
        ],
        compiler_params=pltpu.CompilerParams(vmem_limit_bytes=GRANT),
        name="smooth",
    )(factors, panel, *stay(smoother_gain, smoothed_cov))


def solution(mesh):
    in_specs = (P(None, ("sr", "tm")), P(("sr", "tm"), None), P(("sr", "tm")), P(), P(), P(), P())
    out_specs = (P("tm", None), P(("sr", "tm"), None), P())
    return jax.shard_map(local, mesh=mesh, in_specs=in_specs, out_specs=out_specs, check_vma=False)
```

```python
import functools
import jax
import jax.numpy as jnp
from jax import lax
from jax.experimental import pallas as pl
from jax.experimental.pallas import tpu as pltpu
from jax.sharding import PartitionSpec as P

precise = lax.Precision.HIGHEST
MESH = pl.DeviceIdType.MESH
SLABS = 8
PIVOTS = 4
LAG = 3
GRANT = 24 * 2**20


def dot_high(left, right):
    return jnp.dot(left, right, precision=precise, preferred_element_type=jnp.float32)


def dot_first(left, right):
    return lax.dot_general(
        left, right, (((0,), (0,)), ((), ())), precision=precise, preferred_element_type=jnp.float32
    )


def halves(value):
    high = value.astype(jnp.bfloat16)
    low = (value - high.astype(jnp.float32)).astype(jnp.bfloat16)
    return high, low


def weights(matrix):
    high, low = halves(matrix)
    side = jnp.concatenate([high, low], axis=1)
    return jnp.concatenate([side, side], axis=0)


def times(value, doubled):
    high, low = halves(value)
    width = value.shape[1]
    out = jnp.dot(
        jnp.concatenate([high, low], axis=1), doubled, preferred_element_type=jnp.float32
    )
    return out[:, :width] + out[:, width:]


def gather_kernel(
    blocks, planes, observations, loadings, precision_in, transition_in, filter_cov_in, gain_in,
    drive, panel, precision, transition, filter_cov, gain, small_done,
    tables, out, out_info, rows_in, part, part_info, *scratch,
):
    chips = blocks // 2
    _, _, lows, rows, width = part.shape
    highs = planes // lows
    length, series = panel.shape
    share = part_info.shape[3]
    block = length // blocks
    steps = chips * lows
    tm = lax.axis_index("tm")
    sr = lax.axis_index("sr")
    core = lax.rem(tm, 2)
    chip = tm // 2
    other = 1 - core
    low = lax.rem(sr, lows)
    high = sr // lows
    partner = (2 * chip + other, sr)
    turns = sorted(range(1, chips), key=lambda turn: -turn.bit_count()) + [0]
    order = [turn * lows + half for turn in turns for half in range(lows)[::-1]]
    nearest = order[:-1][::-1]

    def across_to(turn):
        place = 0
        for bit in range((chips - 1).bit_length()):
            mine = lax.rem(chip // 2**bit + turn // 2**bit, 2)
            place = place + mine * 2**bit
        return place

    def across_from(turn):
        return across_to(turn)

    if chips & (chips - 1):

        def across_to(turn):
            return lax.rem(chip + turn, chips)

        def across_from(turn):
            return lax.rem(chip + chips - turn, chips)

    def chip_at(step):
        return across_to(step // lows)

    def low_at(step):
        return lax.rem(low + step % lows, lows)

    def member(step):
        return (2 * chip_at(step) + core, high * lows + low_at(step))

    def mirror(step):
        return (2 * chip_at(step) + other, high * lows + low_at(step))

    def level(step):
        return (tm, lax.rem(high + step, highs) * lows + low)

    loads_done, panel_done = scratch[:2]
    given = (precision_in, transition_in, filter_cov_in, gain_in)
    kept = (precision, transition, filter_cov, gain)
    smalls = [
        pltpu.make_async_copy(source, target, small_done.at[at])
        for at, (source, target) in enumerate(zip(given, kept))
    ]
    for copy in smalls:
        copy.start()
    pieces = loads_done.shape[0]
    depth = series // pieces
    loads = []
    for at in range(pieces):
        here = slice(at * depth, (at + 1) * depth)
        loads.append(
            pltpu.make_async_copy(loadings.at[here, :], rows_in.at[here, :], loads_done.at[at])
        )
        loads[-1].start()
    tall = 2 * block
    panels = {}
    for step in turns:
        start = pl.multiple_of(across_to(step) * tall, tall)
        panels[step] = pltpu.make_async_copy(
            observations.at[pl.ds(start, tall), :],
            panel.at[pl.ds(start, tall), :],
            panel_done.at[step],
        )
        panels[step].start()

    barrier = pltpu.get_barrier_semaphore()
    pl.semaphore_signal(barrier, inc=1, device_id=partner, device_id_type=MESH)
    for step in range(1, steps):
        for device in (member(step), mirror(step)):
            pl.semaphore_signal(barrier, inc=1, device_id=device, device_id_type=MESH)
    for step in range(1, highs):
        pl.semaphore_signal(barrier, inc=1, device_id=level(step), device_id_type=MESH)

    both = None
    weighted = []
    smalls[0].wait()
    for at in range(pieces):
        here = slice(at * depth, (at + 1) * depth)
        columns = [
            jnp.broadcast_to(precision[pl.ds(row, 1), :], (width, width)).T
            for row in range(at * depth // width, (at + 1) * depth // width)
        ]
        loads[at].wait()
        value = rows_in[here, :]
        column = jnp.concatenate(columns, axis=0)
        scaled = value * column
        pair = halves(scaled)
        weighted.append(pair[0])
        top = value.astype(jnp.bfloat16)
        rest = ((value - top.astype(jnp.float32)) * column).astype(jnp.bfloat16)
        each = lax.dot_general(
            top, jnp.concatenate(pair + (rest,), axis=1), (((0,), (0,)), ((), ())),
            preferred_element_type=jnp.float32,
        )
        both = each if both is None else both + each
    weighted = jnp.concatenate(weighted, axis=0)
    info = both[:, :width] + both[:, width : 2 * width] + both[:, 2 * width :].T
    for place in range(2 * steps):
        now = slice(place * share, (place + 1) * share)
        part_info[place // lows % 2, place // (2 * lows), place % lows] = info[now]
    pl.semaphore_wait(barrier, 1 + 2 * (steps - 1) + highs - 1)

    class Stream:
        def __init__(self, part, out, pair_in, mine, cube_in, far_in, pair, across, far, back, last):
            self.part, self.out = part, out
            self.pair_in, self.mine, self.cube_in, self.far_in = pair_in, mine, cube_in, far_in
            self.pair, self.across, self.far, self.back, self.last = pair, across, far, back, last
            self.sent = []
            self.open = {}

        def send(self, key, source, target, semaphores, at, device):
            copy = pltpu.make_async_remote_copy(
                src_ref=source, dst_ref=target,
                send_sem=semaphores.at[0, at], recv_sem=semaphores.at[1, at],
                device_id=device, device_id_type=MESH,
            )
            copy.start()
            self.open[key] = copy
            self.sent.append(copy)

        def wait(self, key):
            self.open[key].wait_recv()

        def to_pair(self, step):
            source = self.part.at[other, chip_at(step), low_at(step)]
            self.send(("pair", step), source, self.pair_in.at[step], self.pair, step, partner)

        def to_cube(self, step):
            self.wait(("pair", step))
            self.mine[step] = self.part[core, chip_at(step), low_at(step)] + self.pair_in[step]
            if step > 0:
                self.send(
                    ("across", step), self.mine.at[step], self.cube_in.at[step],
                    self.across, step, member(step),
                )

        def to_far(self):
            total = self.mine[0]
            for step in nearest:
                self.wait(("across", step))
                total = total + self.cube_in[step]
            self.far_in[high] = total
            for step in range(1, highs):
                self.send(
                    ("far", step), self.far_in.at[high], self.far_in.at[high],
                    self.far, step, level(step),
                )

        def to_back(self, both_cores):
            for step in range(1, highs):
                self.wait(("far", step))
            total = self.far_in[0]
            for step in range(1, highs):
                total = total + self.far_in[step]
            here = self.out.at[core, chip, low]
            here[...] = total
            for step in order[:-1]:
                self.send(("back", step), here, here, self.back, step, member(step))
                if both_cores:
                    self.send(("last", step), here, here, self.last, step, mirror(step))
            self.send(("last", 0), here, here, self.last, 0, partner)

        def to_last(self, step):
            self.wait(("back", step))
            source = across_from(step // lows)
            here = self.out.at[core, source, lax.rem(low + lows - step % lows, lows)]
            self.send(("last", step), here, here, self.last, step, partner)

    small = Stream(part_info, out_info, *scratch[2:11])
    large = Stream(part, out, *scratch[11:20])
    for step in order:
        small.to_pair(step)
    waiting = []
    for turn in turns:
        panels[turn].wait()
        source = across_to(turn)
        start = pl.multiple_of(source * tall, tall)
        proj = jnp.dot(
            panel[pl.ds(start, tall), :], weighted, preferred_element_type=jnp.float32
        )
        for at in range(2):
            for half in range(lows):
                now = slice(at * block + half * rows, at * block + (half + 1) * rows)
                part[at, source, half] = proj[now]
        waiting.append([step for step in order if step // lows == turn])
        for step in waiting[-1]:
            large.to_pair(step)
        if turn == turns[min(2, chips - 1)]:
            for step in order:
                small.to_cube(step)
        if len(waiting) > LAG:
            for step in waiting.pop(0):
                large.to_cube(step)
    for fresh in waiting:
        for step in fresh:
            large.to_cube(step)
    count = length // SLABS
    for copy in smalls[1:]:
        copy.wait()
    small.to_far()
    large.to_far()
    powers(gain[...].T, tables.at[1], count)
    cov_t = weights(filter_cov[...].T)
    coupled = weights(dot_high(gain[...], transition[...]).T)
    small.to_back(True)
    large.to_back(False)
    for step in nearest:
        small.wait(("back", step))
    for step in [0] + nearest:
        small.wait(("last", step))
    places = [
        (at, turn, half) for turn in range(chips) for at in range(2) for half in range(lows)
    ]
    info = jnp.concatenate([out_info[place] for place in places], axis=0)
    closed = transition[...] - dot_high(filter_cov[...], dot_high(info, transition[...]))
    powers(closed.T, tables.at[0], count)
    for step in nearest:
        large.to_last(step)

    def enter(at):
        tall = chips * lows * rows
        given = out[at].reshape(tall, width)
        entered = times(given, cov_t)
        for turn in range(chips):
            for half in range(lows):
                start = pl.multiple_of((2 * turn + at) * block + half * rows, rows)
                now = (turn * lows + half) * rows
                drive[pl.ds(start, rows), :] = entered[now : now + rows]

    enter(core)
    for step in [0] + nearest:
        large.wait(("last", step))
    enter(other)
    slabs = [drive[pl.ds(at, count, stride=SLABS), :] for at in range(SLABS)]
    filtered = scan_slabs(slabs, tables.at[0], False)
    final = lax.broadcasted_iota(jnp.int32, (count, width), 0) == count - 1
    back = [each - times(each, coupled) for each in filtered]
    back[-1] = jnp.where(final, filtered[-1], back[-1])
    smooth = scan_slabs(back, tables.at[1], True)
    for at in range(SLABS):
        drive[pl.ds(at, count, stride=SLABS), :] = smooth[at]
    for stream in (small, large):
        for copy in stream.sent:
            copy.wait_send()


def stay(*arrays):
    return [pltpu.with_memory_space_constraint(array, pltpu.HBM) for array in arrays]


def gather(observations, loadings, noise_precision, transition, filter_cov, gain, blocks, planes):
    length, series = observations.shape
    width = loadings.shape[1]
    chips = blocks // 2
    lows = 2 if planes % 2 == 0 else 1
    highs = planes // lows
    rows = length // (blocks * lows)
    share = width // (blocks * lows)
    pieces = min(4, series // width)
    dma = pltpu.SemaphoreType.DMA
    vmem = pl.BlockSpec(memory_space=pltpu.VMEM)
    hbm = pl.BlockSpec(memory_space=pltpu.HBM)
    steps = chips * lows
    entries = sum(radix - 1 for radix in [SLABS] + radices(length // SLABS))

    def memory(*shape):
        return pltpu.VMEM(shape, jnp.float32)

    def stream(tall):
        return [memory(steps, tall, width)] * 3 + [memory(highs, tall, width)] + (
            [dma((2, steps))] * 2 + [dma((2, highs))] + [dma((2, steps))] * 2
        )

    shapes = [(2, chips, lows, tall, width) for tall in (rows, share)]
    return pl.pallas_call(
        functools.partial(gather_kernel, blocks, planes),
        out_shape=[
            pltpu.VMEM((length, width), jnp.float32),
            pltpu.VMEM((length, series), observations.dtype),
        ],
        in_specs=[hbm] * 6,
        out_specs=[vmem, vmem],
        scratch_shapes=[
            memory(series // width, width),
            memory(width, width),
            memory(width, width),
            memory(width, width),
            dma((4,)),
            pltpu.VMEM((2, entries, 2 * width, 2 * width), jnp.bfloat16),
            memory(*shapes[0]),
            memory(*shapes[1]),
            memory(series, width),
            memory(*shapes[0]),
            memory(*shapes[1]),
            dma((pieces,)),
            dma((chips,)),
        ]
        + stream(share)
        + stream(rows),
        compiler_params=pltpu.CompilerParams(
            collective_id=0, has_side_effects=True, vmem_limit_bytes=GRANT
        ),
        name="gather",
    )(
        *stay(
            observations, loadings, noise_precision.reshape(series // width, width),
            transition, filter_cov, gain,
        )
    )


def shift_rows(value, steps):
    length = value.shape[0]
    row = lax.broadcasted_iota(jnp.int32, value.shape, 0)
    moved = pltpu.roll(value, steps % length, 0)
    keep = row >= steps if steps > 0 else row < length + steps
    return jnp.where(keep, moved, 0.0)


def radices(count):
    bits = (count - 1).bit_length()
    parts = -(-bits // 3)
    return [2 ** (bits * (at + 1) // parts - bits * at // parts) for at in range(parts)][::-1]


def powers(matrix, table, count):
    levels = [SLABS] + radices(count)
    base, start = matrix, 0
    for at, radix in enumerate(levels):
        made = [base]
        top = radix if at + 1 < len(levels) else radix - 1
        table[start] = weights(base)
        while len(made) < top:
            fresh = [dot_high(made[-1], each) for each in made][: top - len(made)]
            for each in fresh:
                if len(made) < radix - 1:
                    table[start + len(made)] = weights(each)
                made.append(each)
        base = made[-1]
        start += radix - 1


def times_many(values, table, start):
    width = values[0].shape[1]
    left = jnp.concatenate([part for value in values for part in halves(value)], axis=1)
    right = table[start : start + len(values)].reshape(2 * width * len(values), 2 * width)
    out = jnp.dot(left, right, preferred_element_type=jnp.float32)
    return out[:, :width] + out[:, width:]


def scan_slabs(slabs, table, reverse):
    order = list(range(SLABS))[::-1] if reverse else list(range(SLABS))
    sign = -1 if reverse else 1
    part = [slabs[now] for now in order]
    ends = part.pop()
    ends = ends + times_many(part[::-1], table, 0)
    start, stride = SLABS - 1, 1
    for radix in radices(ends.shape[0]):
        moved = [shift_rows(ends, sign * stride * at) for at in range(1, radix)]
        ends = ends + times_many(moved, table, start)
        start += radix - 1
        stride *= radix
    size = 1
    while size < SLABS:
        for first in range(size, SLABS - 1, 2 * size):
            for offset in range(min(size, SLABS - 1 - first)):
                add = times(part[first - 1], table[offset])
                part[first + offset] = part[first + offset] + add
        size *= 2
    carry = shift_rows(ends, sign)
    out = [None] * SLABS
    for place, now in enumerate(order[:-1]):
        out[now] = part[place] + times(carry, table[place])
    out[order[-1]] = ends
    return out


def inverse_two(a, b, c):
    scale = 1.0 / (a * c - b * b)
    return c * scale, -b * scale, a * scale


def inverse_four(p):
    e, f, g = inverse_two(p[0][0], p[0][1], p[1][1])
    u00 = e * p[0][2] + f * p[1][2]
    u01 = e * p[0][3] + f * p[1][3]
    u10 = f * p[0][2] + g * p[1][2]
    u11 = f * p[0][3] + g * p[1][3]
    s00 = p[2][2] - (p[0][2] * u00 + p[1][2] * u10)
    s01 = p[2][3] - (p[0][2] * u01 + p[1][2] * u11)
    s11 = p[3][3] - (p[0][3] * u01 + p[1][3] * u11)
    t00, t01, t11 = inverse_two(s00, s01, s11)
    v00 = u00 * t00 + u01 * t01
    v01 = u00 * t01 + u01 * t11
    v10 = u10 * t00 + u11 * t01
    v11 = u10 * t01 + u11 * t11
    a00 = e + (v00 * u00 + v01 * u01)
    a01 = f + (v00 * u10 + v01 * u11)
    a11 = g + (v10 * u10 + v11 * u11)
    return [
        [a00, a01, -v00, -v01],
        [a01, a11, -v10, -v11],
        [-v00, -v10, t00, t01],
        [-v01, -v11, t01, t11],
    ]


def dot_last(left, right):
    return lax.dot_general(left, right, (((1,), (1,)), ((), ())), precision=precise, preferred_element_type=jnp.float32)


def pick(value, lane, half, at):
    index = jnp.where(lane >= half, half + at, at)
    return jnp.take_along_axis(value, index, axis=1, mode="promise_in_bounds")

def sweep(packed):
    half, size = packed.shape
    lane = lax.broadcasted_iota(jnp.int32, (8, size), 1)
    inner = jnp.where(lane >= half, lane - half, lane)
    sub = lax.broadcasted_iota(jnp.int32, (8, size), 0)
    groups = half // 8
    value = [packed[8 * g : 8 * g + 8] for g in range(groups)]

    def spread(tile, at):
        return jnp.broadcast_to(tile[at : at + 1, :], (8, size))

    first = [pick(value[0], lane, half, j) for j in range(PIVOTS)]
    block = [[spread(first[max(i, j)], min(i, j)) for j in range(PIVOTS)] for i in range(PIVOTS)]
    for k in range(0, half, PIVOTS):
        group, place = divmod(k, 8)
        solved = inverse_four(block)
        order = list(range(groups))
        following = k + PIVOTS
        if following < half:
            ahead, spot = divmod(following, 8)
            order.remove(ahead)
            order.insert(0, ahead)
        columns = [None] * groups
        for g in order:
            columns[g] = [pick(value[g], lane, half, k + j) for j in range(PIVOTS)]
            if g == order[0] and following < half:
                coming = [pick(value[g], lane, half, following + j) for j in range(PIVOTS)]
        if following < half:
            moved = [sum(solved[i][j] * columns[ahead][j] for j in range(PIVOTS)) for i in range(PIVOTS)]
            later = []
            for b in range(PIVOTS):
                take = sum(columns[ahead][i] * spread(moved[i], spot + b) for i in range(PIVOTS))
                later.append(coming[b] - take)
            block = [
                [spread(later[max(i, j)], spot + min(i, j)) for j in range(PIVOTS)]
                for i in range(PIVOTS)
            ]
        here = (inner >= k) & (inner < k + PIVOTS)
        rows = []
        for i in range(PIVOTS):
            row = jnp.where(here, 0.0, spread(value[group], place + i))
            rows.append(jnp.where(inner == k + i, 1.0, row))
        fresh = [sum(solved[i][j] * rows[j] for j in range(PIVOTS)) for i in range(PIVOTS)]
        updated = [None] * groups
        for g in order:
            take = sum(columns[g][i] * fresh[i] for i in range(PIVOTS))
            updated[g] = jnp.where(here, 0.0, value[g]) - take
            if g == group:
                for i in range(PIVOTS):
                    updated[g] = jnp.where(sub == place + i, fresh[i], updated[g])
        value = updated
    return jnp.concatenate(value, axis=0)


def invert(matrices, between):
    size = matrices[0].shape[0]
    half = size // 2
    row_at = lax.broadcasted_iota(jnp.int32, (size, size), 0)
    lane_at = lax.broadcasted_iota(jnp.int32, (size, size), 1)
    low = lax.broadcasted_iota(jnp.int32, (half, size), 1) < half
    nothing = jnp.zeros((half, size), jnp.float32)
    diagonal = row_at == lane_at
    scales, scaled = [], []
    for m in matrices:
        only = jnp.where(diagonal, m, 0.0)
        across = lax.rsqrt(jnp.sum(only, axis=0, keepdims=True))
        down = lax.rsqrt(jnp.sum(only, axis=1, keepdims=True))
        scales.append((across, down))
        scaled.append((m * across) * down)
    one, two = scaled
    packed = sweep(jnp.where(low, one[:half], pltpu.roll(two[:half], half, 1)))
    corner = [jnp.where(low, packed, 0.0), jnp.where(low, pltpu.roll(packed, half, 1), 0.0)]
    upper, rest = [], []
    for m, each in zip(scaled, corner):
        over = jnp.where(low, 0.0, dot_high(each, m))
        over = jnp.concatenate([over, nothing], axis=0)
        upper.append(over)
        rest.append(m[half:] - dot_high(jnp.where(low, m[half:], 0.0), over))
    between()
    packed = sweep(jnp.where(low, pltpu.roll(rest[1], half, 1), rest[0]))
    final = [jnp.where(low, 0.0, packed), jnp.where(low, 0.0, pltpu.roll(packed, half, 1))]
    out = []
    for each, over, last, (across, down) in zip(corner, upper, final, scales):
        side = dot_high(over[:half], jnp.concatenate([nothing, last], axis=0))
        top = each + dot_last(side, over) - side
        bottom = last - dot_last(last, over)
        out.append((jnp.concatenate([top, bottom], axis=0) * across) * down)
    return out


def smooth_kernel(
    drive, held, gain_in, cov_in, own, updated, moved_out, gain, cov, staged, split, moved,
    small_done, own_done, moved_done, part_done,
):
    length, width = drive.shape
    smalls = [
        pltpu.make_async_copy(gain_in, gain, small_done.at[0]),
        pltpu.make_async_copy(cov_in, cov, small_done.at[1]),
    ]
    for copy in smalls:
        copy.start()
    block = own.shape[0]
    place = pl.multiple_of(lax.axis_index("tm") * block, block)
    owned = pltpu.make_async_copy(drive.at[pl.ds(place, block), :], own, own_done)
    owned.start()
    whole = drive[...]
    high, rest = halves(whole)
    factors = high.T
    time = lax.broadcasted_iota(jnp.int32, whole.shape, 0)
    kept = halves(jnp.where(time == length - 1, 0.0, whole))
    lag = halves(shift_rows(whole, 1))
    sums = jnp.dot(
        jnp.concatenate([factors, rest.T], axis=0),
        jnp.concatenate(kept + lag, axis=1),
        preferred_element_type=jnp.float32,
    )
    sums = sums[:width] + sums[width:]
    previous = sums[:, :width] + sums[:, width : 2 * width]
    lagged = sums[:, 2 * width : 3 * width] + sums[:, 3 * width :]
    for copy in smalls:
        copy.wait()
    final = whole[length - 8 :, :]
    final = jnp.where(lax.broadcasted_iota(jnp.int32, final.shape, 0) == 7, final, 0.0)
    total = previous + dot_first(final, final)
    total = total + length * cov[...]
    previous = previous + (length - 1) * cov[...]
    lagged = lagged + (length - 1) * dot_high(cov[...], gain[...].T)
    series = held.shape[1]
    parts = [slice(start, min(start + 256, series)) for start in range(0, series, 256)]

    def fill():
        for part in parts:
            cross = jnp.dot(factors, held[:, part], preferred_element_type=jnp.float32).T
            split[part, :] = jnp.concatenate(halves(cross), axis=1)

    total, previous = invert([total, previous], fill)
    total = weights(total)
    moved[...] = dot_high(lagged, previous)
    writes = [owned, pltpu.make_async_copy(moved, moved_out, moved_done)]
    writes[-1].start()
    for at, part in enumerate(parts):
        solved = jnp.dot(split[part, :], total, preferred_element_type=jnp.float32)
        staged[part, :] = solved[:, :width] + solved[:, width:]
        writes.append(
            pltpu.make_async_copy(staged.at[part, :], updated.at[part, :], part_done.at[at])
        )
        writes[-1].start()
    for copy in writes:
        copy.wait()


def local(
    observations, loadings, noise_precision, transition, filter_cov, smoother_gain, smoothed_cov
):
    blocks = lax.axis_size("tm")
    planes = lax.axis_size("sr")
    width = transition.shape[0]
    length = observations.shape[0]
    steps_dev = length // blocks
    factors, panel = gather(
        observations, loadings, noise_precision, transition, filter_cov, smoother_gain,
        blocks, planes,
    )
    vmem = pl.BlockSpec(memory_space=pltpu.VMEM)
    series = observations.shape[1]
    return pl.pallas_call(
        smooth_kernel,
        out_shape=[
            jax.ShapeDtypeStruct((steps_dev, width), jnp.float32),
            jax.ShapeDtypeStruct((series, width), jnp.float32),
            jax.ShapeDtypeStruct((width, width), jnp.float32),
        ],
        in_specs=[vmem] * 2 + [pl.BlockSpec(memory_space=pltpu.HBM)] * 2,
        out_specs=[pl.BlockSpec(memory_space=pltpu.HBM)] * 3,
        scratch_shapes=[
            pltpu.VMEM((width, width), jnp.float32),
            pltpu.VMEM((width, width), jnp.float32),
            pltpu.VMEM((series, width), jnp.float32),
            pltpu.VMEM((series, 2 * width), jnp.bfloat16),
            pltpu.VMEM((width, width), jnp.float32),
            pltpu.SemaphoreType.DMA((2,)),
            pltpu.SemaphoreType.DMA,
            pltpu.SemaphoreType.DMA,
            pltpu.SemaphoreType.DMA((pl.cdiv(series, 256),)),
        ],
        compiler_params=pltpu.CompilerParams(vmem_limit_bytes=GRANT),
        name="smooth",
    )(factors, panel, *stay(smoother_gain, smoothed_cov))


def solution(mesh):
    in_specs = (P(None, ("sr", "tm")), P(("sr", "tm"), None), P(("sr", "tm")), P(), P(), P(), P())
    out_specs = (P("tm", None), P(("sr", "tm"), None), P())
    return jax.shard_map(local, mesh=mesh, in_specs=in_specs, out_specs=out_specs, check_vma=False)
```
